64 devices in a mesh: dp: 4 (over x, y), tp: 16 (over z, core).
Axes of the slice: x: 2, y: 2, z: 8, core: 2. Of those that a mesh axis runs over, the one named last changes fastest.
The devices are a block of a 4x4x8 slice.
Arguments:
- x_in: bfloat16 [4, 4096, 1024], P('dp', 'tp'), parts along dimension 0
- x_mid: bfloat16 [4, 4096, 1024], P('dp', 'tp'), parts along dimension 0
- d_out: bfloat16 [4, 4096, 1024], P('dp', 'tp'), parts along dimension 0
- q_saved: bfloat16 [4, 4096, 16, 64], P('dp', None, 'tp'), parts along dimension 0
- k_saved: bfloat16 [4, 4096, 16, 64], P('dp', None, 'tp'), parts along dimension 0
- v_saved: bfloat16 [4, 4096, 16, 64], P('dp', None, 'tp'), parts along dimension 0
- z_saved: bfloat16 [4, 4096, 4096], P('dp', None, 'tp'), parts along dimension 0
- ln1_gain: float32 [1024], replicated
- ln1_bias: float32 [1024], replicated
- ln2_gain: float32 [1024], replicated
- ln2_bias: float32 [1024], replicated
- w_qkv: bfloat16 [3, 1024, 16, 64], P(None, None, 'tp')
- w_proj: bfloat16 [16, 64, 1024], P('tp')
- w_fc1: bfloat16 [1024, 4096], P(None, 'tp')
- w_fc2: bfloat16 [4096, 1024], P('tp')
Outputs:
- output 1: bfloat16 [4, 4096, 1024], P('dp', 'tp'), parts along dimension 0
- output 2: float32 [12, 1024, 16, 64], P('dp', None, 'tp'), parts along dimension 0
- output 3: float32 [12, 16, 64], P('dp', 'tp'), parts along dimension 0
- output 4: float32 [64, 64, 1024], P(('dp', 'tp')), parts along dimension 0
- output 5: float32 [4096, 4096], P('dp', 'tp'), parts along dimension 0
- output 6: float32 [16384], P(('dp', 'tp')), parts along dimension 0
- output 7: float32 [16384, 1024], P(('dp', 'tp')), parts along dimension 0
- output 8: float32 [24, 1024], P('dp'), parts along dimension 0
There are 4 independent parts. The reference program is written for one: setup_inputs(seed, part) draws one part's arguments, and reference() takes and returns one part's arrays. A program takes and returns all parts, laid end to end along the dimension named above; an argument that names none is the same for every part.
All inputs are finite; a program needn't handle non-finite values.
Results may differ from the reference program's by a relative error of at most 0.0129028.
Values are sent between devices in bfloat16 or wider.
A program may use at most 768 MiB of HBM per device.

```python
import jax
import jax.numpy as jnp
from jax import lax

BATCH_SEQS = 1
SEQ_LEN = 4096
D_MODEL = 1024
N_HEADS = 16
HEAD_DIM = 64
FF_DIM = 4096
LN_EPS = 1e-5
GELU_COEF = 0.044715
GELU_SCALE = 0.7978845608028654


def draw_normal(key, shape, scale):
    return (scale * jax.random.normal(key, shape, jnp.float32)).astype(jnp.bfloat16)


def setup_inputs(seed: int = 0, part: int = 0) -> dict:
    part_keys = jax.random.split(jax.random.fold_in(jax.random.key(seed), part), 7)
    shared_keys = jax.random.split(jax.random.key(seed + 1), 8)
    tok_shape = (BATCH_SEQS, SEQ_LEN, D_MODEL)
    head_shape = (BATCH_SEQS, SEQ_LEN, N_HEADS, HEAD_DIM)
    return {
        'x_in': draw_normal(part_keys[0], tok_shape, 1.0),
        'x_mid': draw_normal(part_keys[1], tok_shape, 1.0),
        'd_out': draw_normal(part_keys[2], tok_shape, 1.0),
        'q_saved': draw_normal(part_keys[3], head_shape, 1.0),
        'k_saved': draw_normal(part_keys[4], head_shape, 1.0),
        'v_saved': draw_normal(part_keys[5], head_shape, 1.0),
        'z_saved': draw_normal(part_keys[6], (BATCH_SEQS, SEQ_LEN, FF_DIM), 1.5),
        'ln1_gain': jax.random.uniform(shared_keys[0], (D_MODEL,), jnp.float32, 0.5, 1.5),
        'ln1_bias': 0.5 * jax.random.normal(shared_keys[1], (D_MODEL,), jnp.float32),
        'ln2_gain': jax.random.uniform(shared_keys[2], (D_MODEL,), jnp.float32, 0.5, 1.5),
        'ln2_bias': 0.5 * jax.random.normal(shared_keys[3], (D_MODEL,), jnp.float32),
        'w_qkv': draw_normal(shared_keys[4], (3, D_MODEL, N_HEADS, HEAD_DIM), D_MODEL ** -0.5),
        'w_proj': draw_normal(shared_keys[5], (N_HEADS, HEAD_DIM, D_MODEL), D_MODEL ** -0.5),
        'w_fc1': draw_normal(shared_keys[6], (D_MODEL, FF_DIM), D_MODEL ** -0.5),
        'w_fc2': draw_normal(shared_keys[7], (FF_DIM, D_MODEL), FF_DIM ** -0.5),
    }


def layer_norm_fwd(token_rows, norm_gain, norm_bias):
    rows_f32 = token_rows.astype(jnp.float32)
    centered = rows_f32 - jnp.mean(rows_f32, axis=-1, keepdims=True)
    inv_std = lax.rsqrt(jnp.mean(centered * centered, axis=-1, keepdims=True) + LN_EPS)
    x_hat = centered * inv_std
    return x_hat, inv_std, (x_hat * norm_gain + norm_bias).astype(jnp.bfloat16)


def layer_norm_bwd(grad_norm, x_hat, inv_std, norm_gain):
    grad_hat = grad_norm * norm_gain
    centered_grad = grad_hat - jnp.mean(grad_hat, axis=-1, keepdims=True)
    return inv_std * (centered_grad - x_hat * jnp.mean(grad_hat * x_hat, axis=-1, keepdims=True))


def gelu_parts(pre_act):
    tanh_val = jnp.tanh(GELU_SCALE * (pre_act + GELU_COEF * pre_act * pre_act * pre_act))
    act_value = 0.5 * pre_act * (1.0 + tanh_val)
    act_slope = 0.5 * (1.0 + tanh_val) + 0.5 * pre_act * (1.0 - tanh_val * tanh_val) * GELU_SCALE * (1.0 + 3.0 * GELU_COEF * pre_act * pre_act)
    return act_value, act_slope


def head_attention_grads(operands):
    q_head, k_head, v_head, dctx_head = operands
    score_scale = HEAD_DIM ** -0.5
    q_wide = q_head.astype(jnp.float32)
    k_wide = k_head.astype(jnp.float32)
    v_wide = v_head.astype(jnp.float32)
    dctx_wide = dctx_head.astype(jnp.float32)
    scores = jnp.einsum('bqe,bke->bqk', q_wide, k_wide) * score_scale
    row_ids = lax.broadcasted_iota(jnp.int32, (SEQ_LEN, SEQ_LEN), 0)
    col_ids = lax.broadcasted_iota(jnp.int32, (SEQ_LEN, SEQ_LEN), 1)
    scores = jnp.where(row_ids >= col_ids, scores, -1e30)
    attn_probs = jax.nn.softmax(scores, axis=-1)
    probs_low = attn_probs.astype(jnp.bfloat16).astype(jnp.float32)
    context = jnp.einsum('bqk,bke->bqe', probs_low, v_wide).astype(jnp.bfloat16)
    grad_probs = jnp.einsum('bqe,bke->bqk', dctx_wide, v_wide)
    grad_scores = attn_probs * (grad_probs - jnp.sum(grad_probs * attn_probs, axis=-1, keepdims=True)) * score_scale
    scores_low = grad_scores.astype(jnp.bfloat16).astype(jnp.float32)
    grad_q = jnp.einsum('bqk,bke->bqe', scores_low, k_wide).astype(jnp.bfloat16)
    grad_k = jnp.einsum('bqk,bqe->bke', scores_low, q_wide).astype(jnp.bfloat16)
    grad_v = jnp.einsum('bqk,bqe->bke', probs_low, dctx_wide).astype(jnp.bfloat16)
    return context, grad_q, grad_k, grad_v


def reference(x_in, x_mid, d_out, q_saved, k_saved, v_saved, z_saved, ln1_gain, ln1_bias, ln2_gain, ln2_bias, w_qkv, w_proj, w_fc1, w_fc2):
    n_tok = BATCH_SEQS * SEQ_LEN
    norm2_hat, norm2_rstd, h2_norm = layer_norm_fwd(x_mid, ln2_gain, ln2_bias)
    act_value, act_slope = gelu_parts(z_saved.astype(jnp.float32))
    dout_rows = d_out.reshape(n_tok, D_MODEL)
    grad_wfc2 = jnp.dot(act_value.astype(jnp.bfloat16).reshape(n_tok, FF_DIM).T, dout_rows, preferred_element_type=jnp.float32)
    grad_act = jnp.dot(dout_rows, w_fc2.T, preferred_element_type=jnp.float32)
    grad_pre = (grad_act * act_slope.reshape(n_tok, FF_DIM)).astype(jnp.bfloat16)
    grad_wfc1 = jnp.dot(h2_norm.reshape(n_tok, D_MODEL).T, grad_pre, preferred_element_type=jnp.float32)
    grad_bfc1 = jnp.sum(grad_pre.astype(jnp.float32), axis=0)
    grad_h2 = jnp.dot(grad_pre, w_fc1.T, preferred_element_type=jnp.float32).reshape(BATCH_SEQS, SEQ_LEN, D_MODEL)
    grad_mid = (d_out.astype(jnp.float32) + layer_norm_bwd(grad_h2, norm2_hat, norm2_rstd, ln2_gain)).astype(jnp.bfloat16)
    mid_rows = grad_mid.reshape(n_tok, D_MODEL)
    grad_ctx = jnp.dot(mid_rows, w_proj.reshape(D_MODEL, D_MODEL).T, preferred_element_type=jnp.float32).astype(jnp.bfloat16)
    grad_ctx = grad_ctx.reshape(BATCH_SEQS, SEQ_LEN, N_HEADS, HEAD_DIM)
    context, grad_q, grad_k, grad_v = lax.map(head_attention_grads, (jnp.moveaxis(q_saved, 2, 0), jnp.moveaxis(k_saved, 2, 0), jnp.moveaxis(v_saved, 2, 0), jnp.moveaxis(grad_ctx, 2, 0)))
    context_rows = jnp.moveaxis(context, 0, 2).reshape(n_tok, D_MODEL)
    grad_wproj = jnp.dot(context_rows.T, mid_rows, preferred_element_type=jnp.float32).reshape(N_HEADS, HEAD_DIM, D_MODEL)
    norm1_hat, norm1_rstd, h1_norm = layer_norm_fwd(x_in, ln1_gain, ln1_bias)
    qkv_rows = jnp.moveaxis(jnp.stack([grad_q, grad_k, grad_v]), 1, 3).reshape(3, n_tok, D_MODEL).astype(jnp.float32)
    grad_wqkv = jnp.einsum('td,ite->ide', h1_norm.reshape(n_tok, D_MODEL).astype(jnp.float32), qkv_rows).reshape(3, D_MODEL, N_HEADS, HEAD_DIM)
    grad_bqkv = jnp.sum(qkv_rows, axis=1).reshape(3, N_HEADS, HEAD_DIM)
    grad_h1 = jnp.einsum('ite,ide->td', qkv_rows, w_qkv.reshape(3, D_MODEL, D_MODEL).astype(jnp.float32)).reshape(BATCH_SEQS, SEQ_LEN, D_MODEL)
    grad_x = (grad_mid.astype(jnp.float32) + layer_norm_bwd(grad_h1, norm1_hat, norm1_rstd, ln1_gain)).astype(jnp.bfloat16)
    grad_vecs = jnp.stack([
        jnp.sum(grad_h1 * norm1_hat, axis=(0, 1)),
        jnp.sum(grad_h1, axis=(0, 1)),
        jnp.sum(grad_h2 * norm2_hat, axis=(0, 1)),
        jnp.sum(grad_h2, axis=(0, 1)),
        jnp.sum(grad_mid.astype(jnp.float32), axis=(0, 1)),
        jnp.sum(d_out.astype(jnp.float32), axis=(0, 1)),
    ])
    return grad_x, grad_wqkv, grad_bqkv, grad_wproj, grad_wfc1, grad_bfc1, grad_wfc2, grad_vecs
```

```python
import functools
import jax, jax.numpy as jnp
from jax import lax
from jax.experimental import pallas as pl
from jax.experimental.pallas import tpu as pltpu
from jax.sharding import PartitionSpec as P

F32, BF16 = jnp.float32, jnp.bfloat16
LOG2E = 1.4426950408889634
LN_EPS = 1e-5
GELU_COEF = 0.044715
GELU_SCALE = 0.7978845608028654


def dot(a, b):
    return lax.dot_general(a, b, (((1,), (0,)), ((), ())), preferred_element_type=F32)


def attn_fwd_kernel(blk, qT, kT, vT, lse_out, ctx_out, sum_out, k_rows, s_buf):
    step = pl.program_id(0)
    dim, seq = kT.shape
    c = (dim ** -0.5) * LOG2E

    @pl.when(step == 0)
    def _():
        def turn(i, _):
            cols = pl.ds(pl.multiple_of(i * blk, blk), blk)
            k_rows[cols, :] = kT[:, cols].T
            return 0
        lax.fori_loop(0, seq // blk, turn, 0)

    q = qT[...]

    def stats(i, carry, masked):
        m, l = carry
        rows = pl.ds(pl.multiple_of(i * blk, blk), blk)
        s = dot(k_rows[rows, :], q) * c
        if masked:
            r = lax.broadcasted_iota(jnp.int32, (blk, blk), 0)
            col = lax.broadcasted_iota(jnp.int32, (blk, blk), 1)
            s = jnp.where(r <= col, s, -1e30)
        s_buf[rows, :] = s
        new = jnp.maximum(m, jnp.max(s, axis=0, keepdims=True))
        l = l * jnp.exp2(m - new) + jnp.sum(jnp.exp2(s - new), axis=0, keepdims=True)
        return new, l

    init = (jnp.full((1, blk), -1e30, F32), jnp.zeros((1, blk), F32))
    carry = lax.fori_loop(0, step, functools.partial(stats, masked=False), init)
    m, l = stats(step, carry, True)
    lse = m + jnp.log2(l)

    def apply(i, carry):
        low_sum, res_sum = carry
        rows = pl.ds(pl.multiple_of(i * blk, blk), blk)
        p = jnp.exp2(s_buf[rows, :] - lse)
        low = p.astype(BF16)
        res = (p - low.astype(F32)).astype(BF16)
        v = vT[:, rows]
        return low_sum + dot(v, low), res_sum + dot(v, res)

    zero = jnp.zeros((dim, blk), F32)
    low_sum, res_sum = lax.fori_loop(0, step + 1, apply, (zero, zero))
    ctx_out[...] = low_sum.astype(BF16)
    sum_out[...] = low_sum + res_sum
    lse_out[...] = jnp.broadcast_to(lse, (8, blk))


def attn_fwd(qT, kT, vT, blk=1024):
    dim, seq = qT.shape
    col = lambda i: (0, i)
    full = lambda i: (0, 0)
    return pl.pallas_call(
        functools.partial(attn_fwd_kernel, blk),
        grid=(seq // blk,),
        in_specs=[pl.BlockSpec((dim, blk), col), pl.BlockSpec((dim, seq), full), pl.BlockSpec((dim, seq), full)],
        out_specs=[pl.BlockSpec((8, blk), col), pl.BlockSpec((dim, blk), col), pl.BlockSpec((dim, blk), col)],
        out_shape=[jax.ShapeDtypeStruct((8, seq), F32), jax.ShapeDtypeStruct((dim, seq), BF16), jax.ShapeDtypeStruct((dim, seq), F32)],
        scratch_shapes=[pltpu.VMEM((seq, dim), BF16), pltpu.VMEM((seq, blk), F32)],
        compiler_params=pltpu.CompilerParams(dimension_semantics=("arbitrary",), vmem_limit_bytes=32 << 20),
        cost_estimate=pl.CostEstimate(flops=3 * seq * seq * 256, bytes_accessed=8 * dim * seq, transcendentals=seq * seq),
        name="attn_fwd",
    )(qT, kT, vT)


def attn_bwd_kernel(blk, qT, kT, vT, dctxT, lse, ctxsum, out, k_rows, dk_acc, dv_acc):
    step = pl.program_id(0)
    last = pl.num_programs(0) - 1
    dim, seq = kT.shape
    scale = dim ** -0.5
    c = scale * LOG2E

    @pl.when(step == 0)
    def _():
        def turn(i, _):
            cols = pl.ds(pl.multiple_of(i * blk, blk), blk)
            k_rows[cols, :] = kT[:, cols].T
            dk_acc[:, cols] = jnp.zeros((dim, blk), F32)
            dv_acc[:, cols] = jnp.zeros((dim, blk), F32)
            return 0
        lax.fori_loop(0, seq // blk, turn, 0)

    qt = qT[...]
    dct = dctxT[...]
    q = qt.T
    dc = dct.T
    delta_row = jnp.sum(dct.astype(F32) * ctxsum[...], axis=0, keepdims=True)
    lse_col = jnp.broadcast_to(lse[0:1, :], (128, blk)).T[:, :1]
    delta_col = jnp.broadcast_to(delta_row, (128, blk)).T[:, :1]

    def block(i, dq, masked):
        cols = pl.ds(pl.multiple_of(i * blk, blk), blk)
        s = dot(q, kT[:, cols]) * c
        dp = dot(dc, vT[:, cols])
        p = jnp.exp2(s - lse_col)
        if masked:
            r = lax.broadcasted_iota(jnp.int32, (blk, blk), 0)
            col = lax.broadcasted_iota(jnp.int32, (blk, blk), 1)
            p = jnp.where(r >= col, p, 0.0)
        ds = (p * (dp - delta_col)).astype(BF16)
        dv_acc[:, cols] += dot(dct, p.astype(BF16))
        dk_acc[:, cols] += dot(qt, ds)
        return dq + dot(ds, k_rows[cols, :])

    dq = lax.fori_loop(0, step, functools.partial(block, masked=False), jnp.zeros((blk, dim), F32))
    dq = block(step, dq, True)
    out[0:dim, pl.ds(pl.multiple_of(step * blk, blk), blk)] = (dq * scale).T.astype(BF16)

    @pl.when(step == last)
    def _():
        def put(i, _):
            cols = pl.ds(pl.multiple_of(i * blk, blk), blk)
            out[dim:2 * dim, cols] = (dk_acc[:, cols] * scale).astype(BF16)
            out[2 * dim:3 * dim, cols] = dv_acc[:, cols].astype(BF16)
            return 0
        lax.fori_loop(0, seq // blk, put, 0)


def attn_bwd(qT, kT, vT, dctxT, lse, ctxsum, blk=512):
    dim, seq = qT.shape
    col = lambda i: (0, i)
    full = lambda i: (0, 0)
    return pl.pallas_call(
        functools.partial(attn_bwd_kernel, blk),
        grid=(seq // blk,),
        in_specs=[pl.BlockSpec((dim, blk), col), pl.BlockSpec((dim, seq), full), pl.BlockSpec((dim, seq), full),
                  pl.BlockSpec((dim, blk), col), pl.BlockSpec((8, blk), col), pl.BlockSpec((dim, blk), col)],
        out_specs=pl.BlockSpec((3 * dim, seq), full),
        out_shape=jax.ShapeDtypeStruct((3 * dim, seq), BF16),
        scratch_shapes=[pltpu.VMEM((seq, dim), BF16), pltpu.VMEM((dim, seq), F32), pltpu.VMEM((dim, seq), F32)],
        compiler_params=pltpu.CompilerParams(dimension_semantics=("arbitrary",), vmem_limit_bytes=40 << 20),
        cost_estimate=pl.CostEstimate(flops=5 * seq * seq * 256, bytes_accessed=14 * dim * seq, transcendentals=seq * seq // 2),
        name="attn_bwd",
    )(qT, kT, vT, dctxT, lse, ctxsum)


def vec_sum_kernel(n, part, out, buf, send_sem, recv_sem):
    me = lax.axis_index('tp')
    barrier = pltpu.get_barrier_semaphore()

    def hello(r, _):
        pl.semaphore_signal(barrier, inc=1, device_id={'tp': lax.rem(me + r, n)}, device_id_type=pl.DeviceIdType.MESH)
        return 0
    lax.fori_loop(1, n, hello, 0)
    pl.semaphore_wait(barrier, n - 1)

    def copy(r):
        return pltpu.make_async_remote_copy(
            src_ref=part, dst_ref=buf.at[me], send_sem=send_sem.at[r], recv_sem=recv_sem.at[me],
            device_id={'tp': lax.rem(me + r, n)}, device_id_type=pl.DeviceIdType.MESH)

    def arrived(r):
        src = lax.rem(me + n - r, n)
        return pltpu.make_async_remote_copy(
            src_ref=part, dst_ref=buf.at[src], send_sem=send_sem.at[r], recv_sem=recv_sem.at[src],
            device_id={'tp': src}, device_id_type=pl.DeviceIdType.MESH)

    def send(r, _):
        copy(r).start()
        return 0
    lax.fori_loop(1, n, send, 0)
    buf[pl.ds(me, 1)] = part[...][None]

    def wait(r, _):
        arrived(r).wait_recv()
        return 0
    lax.fori_loop(1, n, wait, 0)
    out[...] = lax.fori_loop(1, n, lambda j, acc: acc + buf[j], buf[0])

    def drain(r, _):
        copy(r).wait_send()
        return 0
    lax.fori_loop(1, n, drain, 0)


def vec_sum(part, n):
    rows, width = part.shape
    return pl.pallas_call(
        functools.partial(vec_sum_kernel, n),
        in_specs=[pl.BlockSpec(memory_space=pltpu.VMEM)],
        out_specs=pl.BlockSpec(memory_space=pltpu.VMEM),
        out_shape=jax.ShapeDtypeStruct((rows, width), F32),
        scratch_shapes=[pltpu.VMEM((n, rows, width), F32), pltpu.SemaphoreType.DMA((n,)), pltpu.SemaphoreType.DMA((n,))],
        compiler_params=pltpu.CompilerParams(collective_id=1, has_side_effects=True),
        name="vec_sum",
    )(part)


def layer_norm_fwd(token_rows, norm_gain, norm_bias):
    rows_f32 = token_rows.astype(jnp.float32)
    centered = rows_f32 - jnp.mean(rows_f32, axis=-1, keepdims=True)
    inv_std = lax.rsqrt(jnp.mean(centered * centered, axis=-1, keepdims=True) + LN_EPS)
    x_hat = centered * inv_std
    return x_hat, inv_std, (x_hat * norm_gain + norm_bias).astype(jnp.bfloat16)


def layer_norm_bwd(grad_norm, x_hat, inv_std, norm_gain):
    grad_hat = grad_norm * norm_gain
    centered_grad = grad_hat - jnp.mean(grad_hat, axis=-1, keepdims=True)
    return inv_std * (centered_grad - x_hat * jnp.mean(grad_hat * x_hat, axis=-1, keepdims=True))


def gelu_parts(pre_act):
    tanh_val = jnp.tanh(GELU_SCALE * (pre_act + GELU_COEF * pre_act * pre_act * pre_act))
    act_value = 0.5 * pre_act * (1.0 + tanh_val)
    act_slope = 0.5 * (1.0 + tanh_val) + 0.5 * pre_act * (1.0 - tanh_val * tanh_val) * GELU_SCALE * (1.0 + 3.0 * GELU_COEF * pre_act * pre_act)
    return act_value, act_slope


def solution(mesh):
    def local_backward(x_in, x_mid, d_out, q_saved, k_saved, v_saved, z_saved, ln1_gain, ln1_bias, ln2_gain, ln2_bias, w_qkv, w_proj, w_fc1, w_fc2):
        norm2_hat, norm2_rstd, h2_local = layer_norm_fwd(x_mid, ln2_gain, ln2_bias)
        h2_full = lax.all_gather(h2_local, 'tp', axis=1, tiled=True)
        dout_full = lax.all_gather(d_out, 'tp', axis=1, tiled=True)
        act_value, act_slope = gelu_parts(z_saved.astype(jnp.float32))
        grad_wfc2 = jnp.einsum('bsf,bsd->fd', act_value.astype(jnp.bfloat16), dout_full, preferred_element_type=jnp.float32)
        grad_pre = (jnp.einsum('bsd,fd->bsf', dout_full, w_fc2, preferred_element_type=jnp.float32) * act_slope).astype(jnp.bfloat16)
        grad_wfc1 = jnp.einsum('bsd,bsf->df', h2_full, grad_pre, preferred_element_type=jnp.float32)
        grad_bfc1 = jnp.sum(grad_pre, axis=(0, 1), dtype=jnp.float32)
        h2_partial = jnp.einsum('bsf,df->bsd', grad_pre, w_fc1, preferred_element_type=jnp.float32).astype(jnp.bfloat16)
        grad_h2 = lax.psum_scatter(h2_partial, 'tp', scatter_dimension=1, tiled=True).astype(jnp.float32)
        grad_mid = (d_out.astype(jnp.float32) + layer_norm_bwd(grad_h2, norm2_hat, norm2_rstd, ln2_gain)).astype(jnp.bfloat16)
        mid_full = lax.all_gather(grad_mid, 'tp', axis=1, tiled=True)
        norm1_hat, norm1_rstd, h1_local = layer_norm_fwd(x_in, ln1_gain, ln1_bias)
        h1_full = lax.all_gather(h1_local, 'tp', axis=1, tiled=True)
        dim = q_saved.shape[-1]
        seq = q_saved.shape[1]
        q_t, k_t, v_t = (jnp.transpose(a[0, :, 0, :]) for a in (q_saved, k_saved, v_saved))
        lse, ctx_t, ctx_sum = attn_fwd(q_t, k_t, v_t)
        dctx_t = jnp.einsum('ed,sd->es', w_proj[0], mid_full[0], preferred_element_type=jnp.float32).astype(jnp.bfloat16)
        dqkv_t = attn_bwd(q_t, k_t, v_t, dctx_t, lse, ctx_sum)
        grad_wproj = jnp.einsum('es,sd->ed', ctx_t, mid_full[0], preferred_element_type=jnp.float32)[None]
        w_qkv_t = jnp.transpose(w_qkv[:, :, 0, :], (0, 2, 1)).reshape(3 * dim, -1)
        grad_w_t = jnp.einsum('es,sd->ed', dqkv_t, h1_full[0], preferred_element_type=jnp.float32)
        grad_wqkv = jnp.transpose(grad_w_t.reshape(3, dim, -1), (0, 2, 1))[:, :, None, :]
        grad_bqkv = jnp.sum(dqkv_t, axis=1, dtype=jnp.float32).reshape(3, 1, dim)
        h1_partial = jnp.einsum('es,ed->sd', dqkv_t, w_qkv_t, preferred_element_type=jnp.float32).astype(jnp.bfloat16)[None]
        grad_h1 = lax.psum_scatter(h1_partial, 'tp', scatter_dimension=1, tiled=True).astype(jnp.float32)
        grad_x = (grad_mid.astype(jnp.float32) + layer_norm_bwd(grad_h1, norm1_hat, norm1_rstd, ln1_gain)).astype(jnp.bfloat16)
        vec_partial = jnp.stack([
            jnp.sum(grad_h1 * norm1_hat, axis=(0, 1)),
            jnp.sum(grad_h1, axis=(0, 1)),
            jnp.sum(grad_h2 * norm2_hat, axis=(0, 1)),
            jnp.sum(grad_h2, axis=(0, 1)),
            jnp.sum(grad_mid, axis=(0, 1), dtype=jnp.float32),
            jnp.sum(d_out, axis=(0, 1), dtype=jnp.float32),
        ])
        grad_vecs = vec_sum(vec_partial, mesh.shape['tp'])
        return grad_x, grad_wqkv, grad_bqkv, grad_wproj, grad_wfc1, grad_bfc1, grad_wfc2, grad_vecs

    tok_spec = P('dp', 'tp', None)
    head_spec = P('dp', None, 'tp', None)
    in_specs = (tok_spec, tok_spec, tok_spec, head_spec, head_spec, head_spec, P('dp', None, 'tp'),
                P(None), P(None), P(None), P(None),
                P(None, None, 'tp', None), P('tp', None, None), P(None, 'tp'), P('tp', None))
    out_specs = (tok_spec, P('dp', None, 'tp', None), P('dp', 'tp', None), P(('dp', 'tp'), None, None),
                 P('dp', 'tp'), P(('dp', 'tp')), P(('dp', 'tp'), None), P('dp', None))
    return jax.shard_map(local_backward, mesh=mesh, in_specs=in_specs, out_specs=out_specs, check_vma=False)
```

```python
import functools
import jax, jax.numpy as jnp
from jax import lax
from jax.experimental import pallas as pl
from jax.experimental.pallas import tpu as pltpu
from jax.sharding import PartitionSpec as P

F32, BF16 = jnp.float32, jnp.bfloat16
LOG2E = 1.4426950408889634
LN_EPS = 1e-5
GELU_COEF = 0.044715
GELU_SCALE = 0.7978845608028654


def dot(a, b):
    return lax.dot_general(a, b, (((1,), (0,)), ((), ())), preferred_element_type=F32)


def attn_fwd_kernel(blk, qT, kT, vT, lse_out, ctx_out, sum_out, k_rows, s_buf):
    step = pl.program_id(0)
    dim, seq = kT.shape
    c = (dim ** -0.5) * LOG2E

    @pl.when(step == 0)
    def _():
        def turn(i, _):
            cols = pl.ds(pl.multiple_of(i * blk, blk), blk)
            k_rows[cols, :] = kT[:, cols].T
            return 0
        lax.fori_loop(0, seq // blk, turn, 0)

    q = qT[...]

    def stats(i, carry, masked):
        m, l = carry
        rows = pl.ds(pl.multiple_of(i * blk, blk), blk)
        s = dot(k_rows[rows, :], q) * c
        if masked:
            r = lax.broadcasted_iota(jnp.int32, (blk, blk), 0)
            col = lax.broadcasted_iota(jnp.int32, (blk, blk), 1)
            s = jnp.where(r <= col, s, -1e30)
        s_buf[rows, :] = s
        new = jnp.maximum(m, jnp.max(s, axis=0, keepdims=True))
        l = l * jnp.exp2(m - new) + jnp.sum(jnp.exp2(s - new), axis=0, keepdims=True)
        return new, l

    init = (jnp.full((1, blk), -1e30, F32), jnp.zeros((1, blk), F32))
    carry = lax.fori_loop(0, step, functools.partial(stats, masked=False), init)
    m, l = stats(step, carry, True)
    lse = m + jnp.log2(l)

    def apply(i, carry):
        low_sum, res_sum = carry
        rows = pl.ds(pl.multiple_of(i * blk, blk), blk)
        p = jnp.exp2(s_buf[rows, :] - lse)
        low = p.astype(BF16)
        res = (p - low.astype(F32)).astype(BF16)
        v = vT[:, rows]
        return low_sum + dot(v, low), res_sum + dot(v, res)

    zero = jnp.zeros((dim, blk), F32)
    low_sum, res_sum = lax.fori_loop(0, step + 1, apply, (zero, zero))
    ctx_out[...] = low_sum.astype(BF16)
    sum_out[...] = low_sum + res_sum
    lse_out[...] = jnp.broadcast_to(lse, (8, blk))


def attn_fwd(qT, kT, vT, blk=1024):
    dim, seq = qT.shape
    col = lambda i: (0, i)
    full = lambda i: (0, 0)
    return pl.pallas_call(
        functools.partial(attn_fwd_kernel, blk),
        grid=(seq // blk,),
        in_specs=[pl.BlockSpec((dim, blk), col), pl.BlockSpec((dim, seq), full), pl.BlockSpec((dim, seq), full)],
        out_specs=[pl.BlockSpec((8, blk), col), pl.BlockSpec((dim, blk), col), pl.BlockSpec((dim, blk), col)],
        out_shape=[jax.ShapeDtypeStruct((8, seq), F32), jax.ShapeDtypeStruct((dim, seq), BF16), jax.ShapeDtypeStruct((dim, seq), F32)],
        scratch_shapes=[pltpu.VMEM((seq, dim), BF16), pltpu.VMEM((seq, blk), F32)],
        compiler_params=pltpu.CompilerParams(dimension_semantics=("arbitrary",), vmem_limit_bytes=32 << 20),
        cost_estimate=pl.CostEstimate(flops=3 * seq * seq * 256, bytes_accessed=8 * dim * seq, transcendentals=seq * seq),
        name="attn_fwd",
    )(qT, kT, vT)


def attn_bwd_kernel(blk, qT, kT, vT, dctxT, lse, ctxsum, out, k_rows, dk_acc, dv_acc):
    step = pl.program_id(0)
    last = pl.num_programs(0) - 1
    dim, seq = kT.shape
    scale = dim ** -0.5
    c = scale * LOG2E

    @pl.when(step == 0)
    def _():
        def turn(i, _):
            cols = pl.ds(pl.multiple_of(i * blk, blk), blk)
            k_rows[cols, :] = kT[:, cols].T
            dk_acc[:, cols] = jnp.zeros((dim, blk), F32)
            dv_acc[:, cols] = jnp.zeros((dim, blk), F32)
            return 0
        lax.fori_loop(0, seq // blk, turn, 0)

    qt = qT[...]
    dct = dctxT[...]
    q = qt.T
    dc = dct.T
    delta_row = jnp.sum(dct.astype(F32) * ctxsum[...], axis=0, keepdims=True)
    lse_col = jnp.broadcast_to(lse[0:1, :], (128, blk)).T[:, :1]
    delta_col = jnp.broadcast_to(delta_row, (128, blk)).T[:, :1]

    def block(i, dq, masked):
        cols = pl.ds(pl.multiple_of(i * blk, blk), blk)
        s = dot(q, kT[:, cols]) * c
        dp = dot(dc, vT[:, cols])
        p = jnp.exp2(s - lse_col)
        if masked:
            r = lax.broadcasted_iota(jnp.int32, (blk, blk), 0)
            col = lax.broadcasted_iota(jnp.int32, (blk, blk), 1)
            p = jnp.where(r >= col, p, 0.0)
        ds = (p * (dp - delta_col)).astype(BF16)
        dv_acc[:, cols] += dot(dct, p.astype(BF16))
        dk_acc[:, cols] += dot(qt, ds)
        return dq + dot(ds, k_rows[cols, :])

    dq = lax.fori_loop(0, step, functools.partial(block, masked=False), jnp.zeros((blk, dim), F32))
    dq = block(step, dq, True)
    out[0:dim, pl.ds(pl.multiple_of(step * blk, blk), blk)] = (dq * scale).T.astype(BF16)

    @pl.when(step == last)
    def _():
        def put(i, _):
            cols = pl.ds(pl.multiple_of(i * blk, blk), blk)
            out[dim:2 * dim, cols] = (dk_acc[:, cols] * scale).astype(BF16)
            out[2 * dim:3 * dim, cols] = dv_acc[:, cols].astype(BF16)
            return 0
        lax.fori_loop(0, seq // blk, put, 0)


def attn_bwd(qT, kT, vT, dctxT, lse, ctxsum, blk=512):
    dim, seq = qT.shape
    col = lambda i: (0, i)
    full = lambda i: (0, 0)
    return pl.pallas_call(
        functools.partial(attn_bwd_kernel, blk),
        grid=(seq // blk,),
        in_specs=[pl.BlockSpec((dim, blk), col), pl.BlockSpec((dim, seq), full), pl.BlockSpec((dim, seq), full),
                  pl.BlockSpec((dim, blk), col), pl.BlockSpec((8, blk), col), pl.BlockSpec((dim, blk), col)],
        out_specs=pl.BlockSpec((3 * dim, seq), full),
        out_shape=jax.ShapeDtypeStruct((3 * dim, seq), BF16),
        scratch_shapes=[pltpu.VMEM((seq, dim), BF16), pltpu.VMEM((dim, seq), F32), pltpu.VMEM((dim, seq), F32)],
        compiler_params=pltpu.CompilerParams(dimension_semantics=("arbitrary",), vmem_limit_bytes=40 << 20),
        cost_estimate=pl.CostEstimate(flops=5 * seq * seq * 256, bytes_accessed=14 * dim * seq, transcendentals=seq * seq // 2),
        name="attn_bwd",
    )(qT, kT, vT, dctxT, lse, ctxsum)


def layer_norm_fwd(token_rows, norm_gain, norm_bias):
    rows_f32 = token_rows.astype(jnp.float32)
    centered = rows_f32 - jnp.mean(rows_f32, axis=-1, keepdims=True)
    inv_std = lax.rsqrt(jnp.mean(centered * centered, axis=-1, keepdims=True) + LN_EPS)
    x_hat = centered * inv_std
    return x_hat, inv_std, (x_hat * norm_gain + norm_bias).astype(jnp.bfloat16)


def layer_norm_bwd(grad_norm, x_hat, inv_std, norm_gain):
    grad_hat = grad_norm * norm_gain
    centered_grad = grad_hat - jnp.mean(grad_hat, axis=-1, keepdims=True)
    return inv_std * (centered_grad - x_hat * jnp.mean(grad_hat * x_hat, axis=-1, keepdims=True))


def gelu_parts(pre_act):
    tanh_val = jnp.tanh(GELU_SCALE * (pre_act + GELU_COEF * pre_act * pre_act * pre_act))
    act_value = 0.5 * pre_act * (1.0 + tanh_val)
    act_slope = 0.5 * (1.0 + tanh_val) + 0.5 * pre_act * (1.0 - tanh_val * tanh_val) * GELU_SCALE * (1.0 + 3.0 * GELU_COEF * pre_act * pre_act)
    return act_value, act_slope


MESH = pl.DeviceIdType.MESH


def dot_nt(a, b):
    return lax.dot_general(a, b, (((1,), (1,)), ((), ())), preferred_element_type=F32)


def remote(src, dst, send_sem, recv_sem, dev):
    return pltpu.make_async_remote_copy(src_ref=src, dst_ref=dst, send_sem=send_sem, recv_sem=recv_sem,
                                        device_id={'tp': dev}, device_id_type=MESH)


class Place:
    def __init__(self, n, rows):
        me = lax.axis_index('tp')
        self.me, self.n, self.chips, self.half, self.rows = me, n, n // 2, rows // 2, rows
        self.core, self.chip = lax.rem(me, 2), me // 2
        self.partner = me + 1 - 2 * self.core
        self.next = (lax.rem(me + 2, n), lax.rem(me + n - 2, n))

    def origin(self, d, s):
        return lax.rem(self.chip + (self.chips - s if d == 0 else s), self.chips)

    def span(self, d, s, own):
        core = self.core if own else 1 - self.core
        start = (2 * self.origin(d, s) + core) * self.rows + d * self.half
        return pl.ds(pl.multiple_of(start, self.half), self.half)

    def greet(self):
        barrier = pltpu.get_barrier_semaphore()
        for dev in (self.next[0], self.next[1], self.partner):
            pl.semaphore_signal(barrier, inc=1, device_id={'tp': dev}, device_id_type=MESH)
        pl.semaphore_wait(barrier, 3)

    def greet_all(self):
        barrier = pltpu.get_barrier_semaphore()

        def hello(r, _):
            pl.semaphore_signal(barrier, inc=1, device_id={'tp': lax.rem(self.me + r, self.n)}, device_id_type=MESH)
            return 0
        lax.fori_loop(1, self.n, hello, 0)
        pl.semaphore_wait(barrier, self.n - 1)


class Gather:
    def __init__(self, place, buf, send, recv, psend, precv):
        self.p, self.buf, self.send, self.recv, self.psend, self.precv = place, buf, send, recv, psend, precv

    def hop(self, d, s):
        at = self.buf.at[self.p.span(d, s, True)]
        return remote(at, at, self.send.at[d, s], self.recv.at[d, s], self.p.next[d])

    def give(self, d, s):
        at = self.buf.at[self.p.span(d, s, True)]
        return remote(at, at, self.psend.at[d, s], self.precv.at[d, s], self.p.partner)

    def pass_on(self, s, first=False):
        for d in (0, 1):
            if first:
                self.hop(d, s).start()
            else:
                at = self.buf.at[self.p.span(d, s, True)]
                remote(at, at, self.send.at[d, s - 1], self.recv.at[d, s - 1], self.p.next[d]).wait_recv()

                @pl.when(s < self.p.chips - 1)
                def _():
                    self.hop(d, s).start()
            self.give(d, s).start()

    def arrive(self, d, s):
        at = self.buf.at[self.p.span(d, s, False)]
        remote(at, at, self.psend.at[d, s], self.precv.at[d, s], self.p.partner).wait_recv()

    def load(self, d, s):
        return jnp.concatenate([self.buf[self.p.span(d, s, True), :], self.buf[self.p.span(d, s, False), :]], axis=0)

    def drain(self):
        def one(s, _):
            for d in (0, 1):
                self.give(d, s).wait_send()

                @pl.when(s < self.p.chips - 1)
                def _():
                    self.hop(d, s).wait_send()
            return 0
        lax.fori_loop(0, self.p.chips, one, 0)


class Scatter:
    def __init__(self, place, own, keep, out, inc, send, recv, pout, pinc, psend, precv):
        self.p, self.own, self.keep, self.out, self.inc, self.send, self.recv = place, own, keep, out, inc, send, recv
        self.pout, self.pinc, self.psend, self.precv = pout, pinc, psend, precv

    def give(self, d, s):
        return remote(self.pout.at[d, s], self.pinc.at[d, s], self.psend.at[d, s], self.precv.at[d, s], self.p.partner)

    def hop(self, d, r):
        return remote(self.out.at[d, r], self.inc.at[d, r], self.send.at[d, r], self.recv.at[d, r], self.p.next[d])

    def put(self, d, s, part, first=False):
        half = self.p.half
        (self.keep if first else self.own)[d] = part[:half]
        self.pout[d, s] = part[half:].astype(BF16)

    def forward(self, d, s):
        self.give(d, s).wait_recv()

        @pl.when(s >= 2)
        def _():
            self.hop(d, s - 2).wait_recv()
            self.own[d] += self.inc[d, s - 2].astype(F32)
        self.out[d, s - 1] = (self.own[d] + self.pinc[d, s].astype(F32)).astype(BF16)

    def final(self, d):
        last = self.p.chips - 2
        self.give(d, 0).wait_recv()
        self.hop(d, last).wait_recv()
        return self.keep[d] + self.pinc[d, 0].astype(F32) + self.inc[d, last].astype(F32)

    def drain(self):
        def one(s, _):
            for d in (0, 1):
                self.give(d, s).wait_send()

                @pl.when(s < self.p.chips - 1)
                def _():
                    self.hop(d, s).wait_send()
            return 0
        lax.fori_loop(0, self.p.chips, one, 0)


def gather_scratch(n, rows, width):
    sems = [pltpu.SemaphoreType.DMA((2, n // 2))] * 4
    return [pltpu.VMEM((n * rows, width), BF16)] + sems


def scatter_scratch(n, rows, width):
    chips, half = n // 2, rows // 2
    sem = pltpu.SemaphoreType.DMA((2, chips))
    wide = pltpu.VMEM((2, half, width), F32)
    ring = pltpu.VMEM((2, chips - 1, half, width), BF16)
    pair = pltpu.VMEM((2, chips, half, width), BF16)
    return [wide, wide, ring, ring, sem, sem, pair, pair, sem, sem]


def mlp_kernel(n, dout_hbm, dout, x_mid, z, gain, bias, w1, w2, dw1_out, dw2_out, db1_out, dmid_out, vec_out, *scratch):
    gy_s, gh_s, rs_s, (w1_t, w2_t, dw1_t, load_sem) = scratch[:5], scratch[5:10], scratch[10:20], scratch[20:]
    place = Place(n, x_mid.shape[0])
    half = place.half
    gy, gh, rs = Gather(place, *gy_s), Gather(place, *gh_s), Scatter(place, *rs_s)
    mine = pl.ds(pl.multiple_of(place.me * place.rows, place.rows), place.rows)
    load = pltpu.make_async_copy(dout_hbm, gy.buf.at[mine], load_sem)
    load.start()
    place.greet()
    load.wait()
    gy.pass_on(0, True)
    gh.buf[mine, :] = layer_norm_fwd(x_mid[...], gain[...], bias[...])[2]
    w1_t[...] = w1[...].T
    w2_t[...] = w2[...].T
    dw1_t[...] = jnp.zeros_like(dw1_t)
    dw2_out[...] = jnp.zeros_like(dw2_out)
    db1_out[...] = jnp.zeros_like(db1_out)
    gh.pass_on(0, True)

    def block(d, s, first):
        gy.arrive(d, s)
        dy = gy.load(d, s)
        pre = jnp.concatenate([z[place.span(d, s, True), :], z[place.span(d, s, False), :]], axis=0).astype(F32)
        act, slope = gelu_parts(pre)
        dz = (dot(dy, w2_t[...]) * slope).astype(BF16)
        rs.put(d, s, dot(dz, w1_t[...]), first)
        if d == 1:
            rs.give(0, s).start()
        dw2_out[...] += dot(act.astype(BF16).T, dy)
        db1_out[...] += jnp.sum(dz.astype(F32), axis=0, keepdims=True)
        return dz

    def late(d, s, dz):
        gh.arrive(d, s)
        dw1_t[...] += dot(dz.T, gh.load(d, s))

    dz = [block(d, 0, True) for d in (0, 1)]
    rs.give(1, 0).start()
    for d in (0, 1):
        late(d, 0, dz[d])

    def step(s, _):
        gy.pass_on(s)
        dz = [block(d, s, False) for d in (0, 1)]
        rs.give(1, s).start()
        rs.forward(0, s)
        rs.forward(1, s)
        rs.hop(0, s - 1).start()
        gh.pass_on(s)
        rs.hop(1, s - 1).start()
        for d in (0, 1):
            late(d, s, dz[d])
        return 0
    lax.fori_loop(1, place.chips, step, 0)

    vec = jnp.zeros((4, x_mid.shape[1]), F32)
    for d in (0, 1):
        rows = slice(d * half, (d + 1) * half)
        x_hat, inv_std, _ = layer_norm_fwd(x_mid[rows, :], gain[...], bias[...])
        grad = rs.final(d)
        dy = dout[rows, :].astype(F32)
        dmid = (dy + layer_norm_bwd(grad, x_hat, inv_std, gain[...])).astype(BF16)
        dmid_out[rows, :] = dmid
        vec += jnp.concatenate([jnp.sum(a, axis=0, keepdims=True) for a in (grad * x_hat, grad, dmid.astype(F32), dy)], axis=0)
    vec_out[...] = vec
    dw1_out[...] = dw1_t[...].T
    for g in (gy, gh, rs):
        g.drain()


def comm_call(kernel, n, name, cid, args, out_shape, scratch, hbm=()):
    vm = pl.BlockSpec(memory_space=pltpu.VMEM)
    return pl.pallas_call(
        functools.partial(kernel, n),
        in_specs=[pl.BlockSpec(memory_space=pl.ANY) if i in hbm else vm for i in range(len(args))],
        out_specs=[vm] * len(out_shape),
        out_shape=[jax.ShapeDtypeStruct(*o) for o in out_shape],
        scratch_shapes=scratch,
        compiler_params=pltpu.CompilerParams(collective_id=cid, has_side_effects=True, vmem_limit_bytes=63 << 20),
        name=name,
    )(*args)


def mlp_stage(n, dout, x_mid, z, gain, bias, w1, w2):
    rows, width = dout.shape
    units = z.shape[1]
    scratch = gather_scratch(n, rows, width) * 2 + scatter_scratch(n, rows, width) + [
        pltpu.VMEM((units, width), BF16), pltpu.VMEM((width, units), BF16), pltpu.VMEM((units, width), F32), pltpu.SemaphoreType.DMA]
    return comm_call(mlp_kernel, n, "mlp_stage", 1, (dout, dout, x_mid, z, gain, bias, w1, w2),
                     [((width, units), F32), ((units, width), F32), ((1, units), F32), ((rows, width), BF16), ((4, width), F32)], scratch, hbm=(0,))


def mid_kernel(n, dmid_hbm, ctx_t, wo, dctx_out, dwo_out, *scratch):
    g_s, load_sem = scratch[:5], scratch[5]
    place = Place(n, dmid_hbm.shape[0])
    g = Gather(place, *g_s)
    mine = pl.ds(pl.multiple_of(place.me * place.rows, place.rows), place.rows)
    load = pltpu.make_async_copy(dmid_hbm, g.buf.at[mine], load_sem)
    load.start()
    place.greet()
    load.wait()
    g.pass_on(0, True)
    dwo_out[...] = jnp.zeros_like(dwo_out)

    def block(d, s):
        g.arrive(d, s)
        dmid = g.load(d, s)
        dctx = dot_nt(wo[...], dmid).astype(BF16)
        cols = [place.span(d, s, own) for own in (True, False)]
        dctx_out[:, cols[0]] = dctx[:, :place.half]
        dctx_out[:, cols[1]] = dctx[:, place.half:]
        dwo_out[...] += dot(jnp.concatenate([ctx_t[:, c] for c in cols], axis=1), dmid)

    for d in (0, 1):
        block(d, 0)

    def step(s, _):
        g.pass_on(s)
        for d in (0, 1):
            block(d, s)
        return 0
    lax.fori_loop(1, place.chips, step, 0)
    g.drain()


def mid_stage(n, dmid, ctx_t, wo):
    rows, width = dmid.shape
    dim, seq = ctx_t.shape
    return comm_call(mid_kernel, n, "mid_stage", 2, (dmid, ctx_t, wo), [((dim, seq), BF16), ((dim, width), F32)],
                     gather_scratch(n, rows, width) + [pltpu.SemaphoreType.DMA], hbm=(0,))


class Spread:
    def __init__(self, place, part, buf, send, recv):
        self.p, self.part, self.buf, self.send, self.recv = place, part, buf, send, recv

    def to(self, r):
        me = self.p.me
        return remote(self.part, self.buf.at[me], self.send.at[r], self.recv.at[me], lax.rem(me + r, self.p.n))

    def start(self):
        def one(r, _):
            self.to(r).start()
            return 0
        lax.fori_loop(1, self.p.n, one, 0)
        self.buf[pl.ds(self.p.me, 1)] = self.part[...][None]

    def total(self):
        def one(r, _):
            src = lax.rem(self.p.me + self.p.n - r, self.p.n)
            remote(self.part, self.buf.at[src], self.send.at[r], self.recv.at[src], src).wait_recv()
            return 0
        lax.fori_loop(1, self.p.n, one, 0)
        return lax.fori_loop(1, self.p.n, lambda j, acc: acc + self.buf[j], self.buf[0])

    def drain(self):
        def one(r, _):
            self.to(r).wait_send()
            return 0
        lax.fori_loop(1, self.p.n, one, 0)


def qkv_kernel(n, dqkv_t, x_in, dmid, early, gain, bias, w_t, dx_out, dw_out, vec_out, *scratch):
    gh_s, rs_s, (late_part, e_buf, e_send, e_recv, l_buf, l_send, l_recv) = scratch[:5], scratch[5:15], scratch[15:]
    place = Place(n, x_in.shape[0])
    half = place.half
    gh, rs = Gather(place, *gh_s), Scatter(place, *rs_s)
    first_rows, last_rows = Spread(place, early, e_buf, e_send, e_recv), Spread(place, late_part, l_buf, l_send, l_recv)
    mine = pl.ds(pl.multiple_of(place.me * place.rows, place.rows), place.rows)
    gh.buf[mine, :] = layer_norm_fwd(x_in[...], gain[...], bias[...])[2]
    dw_out[...] = jnp.zeros_like(dw_out)
    place.greet_all()

    def cols(d, s):
        return jnp.concatenate([dqkv_t[:, place.span(d, s, own)] for own in (True, False)], axis=1)

    def block(d, s, first):
        rs.put(d, s, dot(cols(d, s).T, w_t[...]), first)
        if d == 1:
            rs.give(0, s).start()

    def late(d, s):
        gh.arrive(d, s)
        dw_out[...] += dot(cols(d, s), gh.load(d, s))

    def scatter_step(s, hold):
        block(0, s, False)
        block(1, s, False)
        rs.give(1, s).start()
        rs.forward(0, s)
        rs.forward(1, s)
        rs.hop(0, s - 1).start()
        if hold:
            gh.pass_on(0, True)
        else:
            gh.pass_on(s - 1)
        rs.hop(1, s - 1).start()
        for d in (0, 1):
            late(d, s - 1)

    scatter_step(1, True)
    first_rows.start()
    block(0, 0, True)
    block(1, 0, True)
    rs.give(1, 0).start()

    def step(s, _):
        scatter_step(s, False)
        return 0
    lax.fori_loop(2, place.chips, step, 0)
    gh.pass_on(place.chips - 1)

    vec = jnp.zeros((2, x_in.shape[1]), F32)
    for d in (0, 1):
        rows = slice(d * half, (d + 1) * half)
        x_hat, inv_std, _ = layer_norm_fwd(x_in[rows, :], gain[...], bias[...])
        grad = rs.final(d)
        dx_out[rows, :] = (dmid[rows, :].astype(F32) + layer_norm_bwd(grad, x_hat, inv_std, gain[...])).astype(BF16)
        vec += jnp.concatenate([jnp.sum(grad * x_hat, axis=0, keepdims=True), jnp.sum(grad, axis=0, keepdims=True)], axis=0)
    late_part[...] = vec
    for d in (0, 1):
        late(d, place.chips - 1)
    last_rows.start()
    vec_out[2:6, :] = first_rows.total()
    vec_out[0:2, :] = last_rows.total()
    for g in (gh, rs, first_rows, last_rows):
        g.drain()


def qkv_stage(n, dqkv_t, x_in, dmid, early, gain, bias, w_t):
    rows, width = x_in.shape
    sem = pltpu.SemaphoreType.DMA((n,))
    scratch = gather_scratch(n, rows, width) + scatter_scratch(n, rows, width) + [
        pltpu.VMEM((2, width), F32), pltpu.VMEM((n, 4, width), F32), sem, sem, pltpu.VMEM((n, 2, width), F32), sem, sem]
    return comm_call(qkv_kernel, n, "qkv_stage", 3, (dqkv_t, x_in, dmid, early, gain, bias, w_t),
                     [((rows, width), BF16), (w_t.shape, F32), ((6, width), F32)], scratch)


def solution(mesh):
    def local_backward(x_in, x_mid, d_out, q_saved, k_saved, v_saved, z_saved, ln1_gain, ln1_bias, ln2_gain, ln2_bias, w_qkv, w_proj, w_fc1, w_fc2):
        n = mesh.shape['tp']
        dim = q_saved.shape[-1]
        row = lambda a: a[None, :]
        q_t, k_t, v_t = (jnp.transpose(a[0, :, 0, :]) for a in (q_saved, k_saved, v_saved))
        lse, ctx_t, ctx_sum = attn_fwd(q_t, k_t, v_t)
        grad_wfc1, grad_wfc2, grad_bfc1, grad_mid, early = mlp_stage(n, d_out[0], x_mid[0], z_saved[0], row(ln2_gain), row(ln2_bias), w_fc1, w_fc2)
        dctx_t, grad_wproj = mid_stage(n, grad_mid, ctx_t, w_proj[0])
        dqkv_t = attn_bwd(q_t, k_t, v_t, dctx_t, lse, ctx_sum)
        w_qkv_t = jnp.transpose(w_qkv[:, :, 0, :], (0, 2, 1)).reshape(3 * dim, -1)
        grad_x, grad_w_t, grad_vecs = qkv_stage(n, dqkv_t, x_in[0], grad_mid, early, row(ln1_gain), row(ln1_bias), w_qkv_t)
        grad_wqkv = jnp.transpose(grad_w_t.reshape(3, dim, -1), (0, 2, 1))[:, :, None, :]
        grad_bqkv = jnp.sum(dqkv_t, axis=1, dtype=jnp.float32).reshape(3, 1, dim)
        return grad_x[None], grad_wqkv, grad_bqkv, grad_wproj[None], grad_wfc1, grad_bfc1[0], grad_wfc2, grad_vecs

    tok_spec = P('dp', 'tp', None)
    head_spec = P('dp', None, 'tp', None)
    in_specs = (tok_spec, tok_spec, tok_spec, head_spec, head_spec, head_spec, P('dp', None, 'tp'),
                P(None), P(None), P(None), P(None),
                P(None, None, 'tp', None), P('tp', None, None), P(None, 'tp'), P('tp', None))
    out_specs = (tok_spec, P('dp', None, 'tp', None), P('dp', 'tp', None), P(('dp', 'tp'), None, None),
                 P('dp', 'tp'), P(('dp', 'tp')), P(('dp', 'tp'), None), P('dp', None))
    return jax.shard_map(local_backward, mesh=mesh, in_specs=in_specs, out_specs=out_specs, check_vma=False)
```

```python
import functools
import jax, jax.numpy as jnp
from jax import lax
from jax.experimental import pallas as pl
from jax.experimental.pallas import tpu as pltpu
from jax.sharding import PartitionSpec as P

F32, BF16 = jnp.float32, jnp.bfloat16
LOG2E = 1.4426950408889634
LN_EPS = 1e-5
GELU_COEF = 0.044715
GELU_SCALE = 0.7978845608028654


def dot(a, b):
    return lax.dot_general(a, b, (((1,), (0,)), ((), ())), preferred_element_type=F32)


def layer_norm_fwd(token_rows, norm_gain, norm_bias):
    rows_f32 = token_rows.astype(jnp.float32)
    centered = rows_f32 - jnp.mean(rows_f32, axis=-1, keepdims=True)
    inv_std = lax.rsqrt(jnp.mean(centered * centered, axis=-1, keepdims=True) + LN_EPS)
    x_hat = centered * inv_std
    return x_hat, inv_std, (x_hat * norm_gain + norm_bias).astype(jnp.bfloat16)


def layer_norm_bwd(grad_norm, x_hat, inv_std, norm_gain):
    grad_hat = grad_norm * norm_gain
    centered_grad = grad_hat - jnp.mean(grad_hat, axis=-1, keepdims=True)
    return inv_std * (centered_grad - x_hat * jnp.mean(grad_hat * x_hat, axis=-1, keepdims=True))


def gelu_parts(pre_act):
    tanh_val = jnp.tanh(GELU_SCALE * (pre_act + GELU_COEF * pre_act * pre_act * pre_act))
    act_value = 0.5 * pre_act * (1.0 + tanh_val)
    act_slope = 0.5 * (1.0 + tanh_val) + 0.5 * pre_act * (1.0 - tanh_val * tanh_val) * GELU_SCALE * (1.0 + 3.0 * GELU_COEF * pre_act * pre_act)
    return act_value, act_slope


def attn_stats(step, blk, qT, kT, vT, k_rows, s_buf, lse_out, ctx_out, sum_out):
    dim, seq = kT.shape
    c = (dim ** -0.5) * LOG2E
    here = pl.ds(pl.multiple_of(step * blk, blk), blk)
    q = qT[:, here]
    k_rows[here, :] = kT[:, here].T

    def stats(i, carry, masked):
        m, l = carry
        rows = pl.ds(pl.multiple_of(i * blk, blk), blk)
        s = dot(k_rows[rows, :], q) * c
        if masked:
            r = lax.broadcasted_iota(jnp.int32, (blk, blk), 0)
            col = lax.broadcasted_iota(jnp.int32, (blk, blk), 1)
            s = jnp.where(r <= col, s, -1e30)
        s_buf[rows, :] = s
        new = jnp.maximum(m, jnp.max(s, axis=0, keepdims=True))
        l = l * jnp.exp2(m - new) + jnp.sum(jnp.exp2(s - new), axis=0, keepdims=True)
        return new, l

    init = (jnp.full((1, blk), -1e30, F32), jnp.zeros((1, blk), F32))
    carry = lax.fori_loop(0, step, functools.partial(stats, masked=False), init)
    m, l = stats(step, carry, True)
    lse = m + jnp.log2(l)

    def apply(i, carry):
        low_sum, res_sum = carry
        rows = pl.ds(pl.multiple_of(i * blk, blk), blk)
        p = jnp.exp2(s_buf[rows, :] - lse)
        low = p.astype(BF16)
        res = (p - low.astype(F32)).astype(BF16)
        v = vT[:, rows]
        return low_sum + dot(v, low), res_sum + dot(v, res)

    zero = jnp.zeros((dim, blk), F32)
    low_sum, res_sum = lax.fori_loop(0, step + 1, apply, (zero, zero))
    ctx_out[:, here] = low_sum.astype(BF16)
    sum_out[:, here] = low_sum + res_sum
    lse_out[:, here] = jnp.broadcast_to(lse, (8, blk))


def attn_grads(blk, qT, kT, vT, dctxT, lse, ctxsum, out, k_rows, dk_acc, dv_acc, service):
    dim, seq = kT.shape
    scale = dim ** -0.5
    c = scale * LOG2E

    def turn(i, _):
        cols = pl.ds(pl.multiple_of(i * blk, blk), blk)
        k_rows[cols, :] = kT[:, cols].T
        dk_acc[:, cols] = jnp.zeros((dim, blk), F32)
        dv_acc[:, cols] = jnp.zeros((dim, blk), F32)
        return 0
    lax.fori_loop(0, seq // blk, turn, 0)

    def queries(step, _):
        here = pl.ds(pl.multiple_of(step * blk, blk), blk)
        qt = qT[:, here]
        dct = dctxT[:, here]
        q = qt.T
        dc = dct.T
        delta_row = jnp.sum(dct.astype(F32) * ctxsum[:, here], axis=0, keepdims=True)
        lse_col = jnp.broadcast_to(lse[0:1, here], (128, blk)).T[:, :1]
        delta_col = jnp.broadcast_to(delta_row, (128, blk)).T[:, :1]
        base = step * (step + 1) // 2

        def block(i, dq, masked):
            service(base + i)
            cols = pl.ds(pl.multiple_of(i * blk, blk), blk)
            s = dot(q, kT[:, cols]) * c
            dp = dot(dc, vT[:, cols])
            p = jnp.exp2(s - lse_col)
            if masked:
                r = lax.broadcasted_iota(jnp.int32, (blk, blk), 0)
                col = lax.broadcasted_iota(jnp.int32, (blk, blk), 1)
                p = jnp.where(r >= col, p, 0.0)
            ds = (p * (dp - delta_col)).astype(BF16)
            dv_acc[:, cols] += dot(dct, p.astype(BF16))
            dk_acc[:, cols] += dot(qt, ds)
            return dq + dot(ds, k_rows[cols, :])

        dq = lax.fori_loop(0, step, functools.partial(block, masked=False), jnp.zeros((blk, dim), F32))
        dq = block(step, dq, True)
        out[0:dim, here] = (dq * scale).T.astype(BF16)
        return 0
    lax.fori_loop(0, seq // blk, queries, 0)

    def put(i, _):
        cols = pl.ds(pl.multiple_of(i * blk, blk), blk)
        out[dim:2 * dim, cols] = (dk_acc[:, cols] * scale).astype(BF16)
        out[2 * dim:3 * dim, cols] = dv_acc[:, cols].astype(BF16)
        return 0
    lax.fori_loop(0, seq // blk, put, 0)


MESH = pl.DeviceIdType.MESH
SUBS = 2


def dot_nt(a, b):
    return lax.dot_general(a, b, (((1,), (1,)), ((), ())), preferred_element_type=F32)


def remote(src, dst, send_sem, recv_sem, dev):
    return pltpu.make_async_remote_copy(src_ref=src, dst_ref=dst, send_sem=send_sem, recv_sem=recv_sem,
                                        device_id={'tp': dev}, device_id_type=MESH)


class Place:
    def __init__(self, n, rows):
        me = lax.axis_index('tp')
        self.me, self.n, self.chips, self.half, self.rows = me, n, n // 2, rows // 2, rows
        self.core, self.chip = lax.rem(me, 2), me // 2
        self.partner = me + 1 - 2 * self.core
        self.next = (lax.rem(me + 2, n), lax.rem(me + n - 2, n))
        self.sub = self.half // SUBS

    def origin(self, d, s):
        return lax.rem(self.chip + (self.chips - s if d == 0 else s), self.chips)

    def span(self, d, s, own):
        core = self.core if own else 1 - self.core
        start = (2 * self.origin(d, s) + core) * self.rows + d * self.half
        return pl.ds(pl.multiple_of(start, self.half), self.half)

    def part(self, d, s, own, sub):
        core = self.core if own else 1 - self.core
        start = (2 * self.origin(d, s) + core) * self.rows + d * self.half + sub * self.sub
        return pl.ds(pl.multiple_of(start, self.sub), self.sub)

    def greet(self):
        barrier = pltpu.get_barrier_semaphore()
        for dev in (self.next[0], self.next[1], self.partner):
            pl.semaphore_signal(barrier, inc=1, device_id={'tp': dev}, device_id_type=MESH)
        pl.semaphore_wait(barrier, 3)

    def greet_all(self):
        barrier = pltpu.get_barrier_semaphore()

        def hello(r, _):
            pl.semaphore_signal(barrier, inc=1, device_id={'tp': lax.rem(self.me + r, self.n)}, device_id_type=MESH)
            return 0
        lax.fori_loop(1, self.n, hello, 0)
        pl.semaphore_wait(barrier, self.n - 1)


class Gather:
    def __init__(self, place, buf, send, recv, psend, precv):
        self.p, self.buf, self.send, self.recv, self.psend, self.precv = place, buf, send, recv, psend, precv

    def hop(self, d, s, sub):
        at = self.buf.at[self.p.part(d, s, True, sub)]
        return remote(at, at, self.send.at[d, s, sub], self.recv.at[d, s, sub], self.p.next[d])

    def give(self, d, s, sub):
        at = self.buf.at[self.p.part(d, s, True, sub)]
        return remote(at, at, self.psend.at[d, s, sub], self.precv.at[d, s, sub], self.p.partner)

    def first(self):
        for sub in range(SUBS):
            for d in (0, 1):
                self.hop(d, 0, sub).start()
        for sub in range(SUBS):
            for d in (0, 1):
                self.give(d, 0, sub).start()

    def pass_one(self, s, sub):
        for d in (0, 1):
            at = self.buf.at[self.p.part(d, s, True, sub)]
            remote(at, at, self.send.at[d, s - 1, sub], self.recv.at[d, s - 1, sub], self.p.next[d]).wait_recv()

            @pl.when(s < self.p.chips - 1)
            def _():
                self.hop(d, s, sub).start()
            self.give(d, s, sub).start()

    def pass_on(self, s):
        for sub in range(SUBS):
            self.pass_one(s, sub)

    def arrive(self, d, s):
        for sub in range(SUBS):
            at = self.buf.at[self.p.part(d, s, False, sub)]
            remote(at, at, self.psend.at[d, s, sub], self.precv.at[d, s, sub], self.p.partner).wait_recv()

    def load(self, d, s):
        return jnp.concatenate([self.buf[self.p.span(d, s, True), :], self.buf[self.p.span(d, s, False), :]], axis=0)

    def drain(self):
        def one(s, _):
            for d in (0, 1):
                for sub in range(SUBS):
                    self.give(d, s, sub).wait_send()

                    @pl.when(s < self.p.chips - 1)
                    def _():
                        self.hop(d, s, sub).wait_send()
            return 0
        lax.fori_loop(0, self.p.chips, one, 0)


class Scatter:
    def __init__(self, place, own, keep, out, inc, send, recv, pout, pinc, psend, precv):
        self.p, self.own, self.keep, self.out, self.inc, self.send, self.recv = place, own, keep, out, inc, send, recv
        self.pout, self.pinc, self.psend, self.precv = pout, pinc, psend, precv

    def give(self, d, s):
        return remote(self.pout.at[d, s], self.pinc.at[d, s], self.psend.at[d, s], self.precv.at[d, s], self.p.partner)

    def hop(self, d, r, sub):
        rows = slice(sub * self.p.sub, (sub + 1) * self.p.sub)
        return remote(self.out.at[d, r, rows], self.inc.at[d, r, rows], self.send.at[d, r, sub], self.recv.at[d, r, sub], self.p.next[d])

    def put(self, d, s, part, first=False):
        half = self.p.half
        (self.keep if first else self.own)[d] = part[:half]
        self.pout[d, s] = part[half:].astype(BF16)

    def join(self, d, s):
        self.give(d, s).wait_recv()
        self.own[d] += self.pinc[d, s].astype(F32)

    def forward(self, d, s, sub):
        rows = slice(sub * self.p.sub, (sub + 1) * self.p.sub)

        @pl.when(s >= 2)
        def _():
            self.hop(d, s - 2, sub).wait_recv()
            self.out[d, s - 1, rows] = (self.own[d, rows] + self.inc[d, s - 2, rows].astype(F32)).astype(BF16)

        @pl.when(s < 2)
        def _():
            self.out[d, s - 1, rows] = self.own[d, rows].astype(BF16)

    def pass_on(self, s):
        for d in (0, 1):
            self.join(d, s)
        before = None
        for sub in range(SUBS):
            for d in (0, 1):
                self.forward(d, s, sub)
                if before is not None:
                    self.hop(*before).start()
                before = (d, s - 1, sub)
        return self.hop(*before)

    def final(self, d, store):
        last = self.p.chips - 2
        self.give(d, 0).wait_recv()
        for sub in range(SUBS):
            self.hop(d, last, sub).wait_recv()
        return store[d] + self.pinc[d, 0].astype(F32) + self.inc[d, last].astype(F32)

    def drain(self):
        def one(s, _):
            for d in (0, 1):
                self.give(d, s).wait_send()
                for sub in range(SUBS):
                    @pl.when(s < self.p.chips - 1)
                    def _():
                        self.hop(d, s, sub).wait_send()
            return 0
        lax.fori_loop(0, self.p.chips, one, 0)


def gather_scratch(n, rows, width):
    sems = [pltpu.SemaphoreType.DMA((2, n // 2, SUBS))] * 4
    return [pltpu.VMEM((n * rows, width), BF16)] + sems


def scatter_scratch(n, rows, width):
    chips, half = n // 2, rows // 2
    sem = pltpu.SemaphoreType.DMA((2, chips))
    fine = pltpu.SemaphoreType.DMA((2, chips, SUBS))
    wide = pltpu.VMEM((2, half, width), F32)
    ring = pltpu.VMEM((2, chips - 1, half, width), BF16)
    pair = pltpu.VMEM((2, chips, half, width), BF16)
    return [wide, wide, ring, ring, fine, fine, pair, pair, sem, sem]


def mlp_kernel(n, dout_hbm, dout, x_mid, z, gain, bias, w1, w2, qT, kT, vT,
               dw1_out, dw2_out, db1_out, dmid_out, vec_out, lse_out, ctx_out, sum_out, *scratch):
    gy_s, gh_s, rs_s, (w1_t, w2_t, dw1_t, load_sem, k_rows, s_buf) = scratch[:5], scratch[5:10], scratch[10:20], scratch[20:]
    place = Place(n, x_mid.shape[0])
    half = place.half
    blk = kT.shape[1] // place.chips
    gy, gh, rs = Gather(place, *gy_s), Gather(place, *gh_s), Scatter(place, *rs_s)
    mine = pl.ds(pl.multiple_of(place.me * place.rows, place.rows), place.rows)
    load = pltpu.make_async_copy(dout_hbm, gy.buf.at[mine], load_sem)
    load.start()
    place.greet()
    load.wait()
    gy.first()
    gh.buf[mine, :] = layer_norm_fwd(x_mid[...], gain[...], bias[...])[2]
    w1_t[...] = w1[...].T
    w2_t[...] = w2[...].T
    dw1_t[...] = jnp.zeros_like(dw1_t)
    dw2_out[...] = jnp.zeros_like(dw2_out)
    db1_out[...] = jnp.zeros_like(db1_out)
    gh.first()

    def block(d, s, first):
        gy.arrive(d, s)
        dy = gy.load(d, s)
        pre = jnp.concatenate([z[place.span(d, s, True), :], z[place.span(d, s, False), :]], axis=0).astype(F32)
        act, slope = gelu_parts(pre)
        dz = (dot(dy, w2_t[...]) * slope).astype(BF16)
        rs.put(d, s, dot(dz, w1_t[...]), first)
        if d == 1:
            rs.give(0, s).start()
        dw2_out[...] += dot(act.astype(BF16).T, dy)
        db1_out[...] += jnp.sum(dz.astype(F32), axis=0, keepdims=True)
        return dz

    def late(d, s, dz):
        gh.arrive(d, s)
        dw1_t[...] += dot(dz.T, gh.load(d, s))

    def attend(s):
        attn_stats(s, blk, qT, kT, vT, k_rows, s_buf, lse_out, ctx_out, sum_out)

    dz = [block(d, 0, True) for d in (0, 1)]
    rs.give(1, 0).start()
    for d in (0, 1):
        late(d, 0, dz[d])
    attend(0)

    def step(s, _):
        gy.pass_on(s)
        dz = [block(d, s, False) for d in (0, 1)]
        rs.give(1, s).start()
        tail = rs.pass_on(s)
        gh.pass_on(s)
        tail.start()
        for d in (0, 1):
            late(d, s, dz[d])
        attend(s)
        return 0
    lax.fori_loop(1, place.chips, step, 0)
    dw1_out[...] = dw1_t[...].T

    vec = jnp.zeros((4, x_mid.shape[1]), F32)
    for d in (0, 1):
        rows = slice(d * half, (d + 1) * half)
        x_hat, inv_std, _ = layer_norm_fwd(x_mid[rows, :], gain[...], bias[...])
        grad = rs.final(d, rs.keep)
        dy = dout[rows, :].astype(F32)
        dmid = (dy + layer_norm_bwd(grad, x_hat, inv_std, gain[...])).astype(BF16)
        dmid_out[rows, :] = dmid
        vec += jnp.concatenate([jnp.sum(a, axis=0, keepdims=True) for a in (grad * x_hat, grad, dmid.astype(F32), dy)], axis=0)
    vec_out[...] = vec
    for g in (gy, gh, rs):
        g.drain()


def comm_call(kernel, n, name, cid, args, out_shape, scratch, limit, hbm=()):
    vm = pl.BlockSpec(memory_space=pltpu.VMEM)
    return pl.pallas_call(
        functools.partial(kernel, n),
        in_specs=[pl.BlockSpec(memory_space=pl.ANY) if i in hbm else vm for i in range(len(args))],
        out_specs=[vm] * len(out_shape),
        out_shape=[jax.ShapeDtypeStruct(*o) for o in out_shape],
        scratch_shapes=scratch,
        compiler_params=pltpu.CompilerParams(collective_id=cid, has_side_effects=True, vmem_limit_bytes=limit << 20),
        name=name,
    )(*args)


def mlp_stage(n, dout, x_mid, z, gain, bias, w1, w2, q_t, k_t, v_t):
    rows, width = dout.shape
    units = z.shape[1]
    dim, seq = q_t.shape
    scratch = gather_scratch(n, rows, width) * 2 + scatter_scratch(n, rows, width) + [
        pltpu.VMEM((units, width), BF16), pltpu.VMEM((width, units), BF16), pltpu.VMEM((units, width), F32), pltpu.SemaphoreType.DMA,
        pltpu.VMEM((seq, dim), BF16), pltpu.VMEM((seq, 2 * seq // n), F32)]
    return comm_call(mlp_kernel, n, "mlp_stage", 1, (dout, dout, x_mid, z, gain, bias, w1, w2, q_t, k_t, v_t),
                     [((width, units), F32), ((units, width), F32), ((1, units), F32), ((rows, width), BF16), ((4, width), F32),
                      ((8, seq), F32), ((dim, seq), BF16), ((dim, seq), F32)], scratch, 63, hbm=(0,))


class Spread:
    def __init__(self, place, part, buf, send, recv):
        self.p, self.part, self.buf, self.send, self.recv = place, part, buf, send, recv

    def to(self, r):
        me = self.p.me
        return remote(self.part, self.buf.at[me], self.send.at[r], self.recv.at[me], lax.rem(me + r, self.p.n))

    def start(self):
        def one(r, _):
            self.to(r).start()
            return 0
        lax.fori_loop(1, self.p.n, one, 0)
        self.buf[pl.ds(self.p.me, 1)] = self.part[...][None]

    def total(self):
        def one(r, _):
            src = lax.rem(self.p.me + self.p.n - r, self.p.n)
            remote(self.part, self.buf.at[src], self.send.at[r], self.recv.at[src], src).wait_recv()
            return 0
        lax.fori_loop(1, self.p.n, one, 0)
        return lax.fori_loop(1, self.p.n, lambda j, acc: acc + self.buf[j], self.buf[0])

    def drain(self):
        def one(r, _):
            self.to(r).wait_send()
            return 0
        lax.fori_loop(1, self.p.n, one, 0)


def attn_kernel(n, dmid_hbm, dmid, ctx_t, ctx_sum, lse, qT, kT, vT, wo, x_in, early, gain, bias, w_t,
                dwo_out, dx_out, dw_out, db_out, vec_out, *scratch):
    g_s, gh_s, rs_s = scratch[:5], scratch[5:10], scratch[10:20]
    load_sem, dctx, dqkv_t, k_rows, dk_acc, dv_acc, late_part, e_buf, e_send, e_recv, l_buf, l_send, l_recv = scratch[20:]
    place = Place(n, x_in.shape[0])
    half, chips = place.half, place.chips
    seq = kT.shape[1]
    blk = seq // chips
    g, gh, rs = Gather(place, *g_s), Gather(place, *gh_s), Scatter(place, *rs_s)
    first_rows, last_rows = Spread(place, early, e_buf, e_send, e_recv), Spread(place, late_part, l_buf, l_send, l_recv)
    mine = pl.ds(pl.multiple_of(place.me * place.rows, place.rows), place.rows)
    load = pltpu.make_async_copy(dmid_hbm, g.buf.at[mine], load_sem)
    load.start()
    place.greet_all()
    load.wait()
    g.first()
    gh.buf[mine, :] = layer_norm_fwd(x_in[...], gain[...], bias[...])[2]
    dwo_out[...] = jnp.zeros_like(dwo_out)
    dw_out[...] = jnp.zeros_like(dw_out)
    db_out[...] = jnp.zeros_like(db_out)

    def project(d, s):
        g.arrive(d, s)
        rows = g.load(d, s)
        both = dot_nt(wo[...], rows).astype(BF16)
        cols = [place.span(d, s, own) for own in (True, False)]
        dctx[:, cols[0]] = both[:, :half]
        dctx[:, cols[1]] = both[:, half:]
        dwo_out[...] += dot(jnp.concatenate([ctx_t[:, c] for c in cols], axis=1), rows)

    for d in (0, 1):
        project(d, 0)

    def mid_step(s, _):
        g.pass_on(s)
        for d in (0, 1):
            project(d, s)
        return 0
    lax.fori_loop(1, chips - 1, mid_step, 0)
    g.pass_on(chips - 1)
    gh.first()
    first_rows.start()
    for d in (0, 1):
        project(d, chips - 1)

    stride = 3
    blocks = chips * (chips + 1) // 2
    done = (blocks + stride - 1) // stride
    events = SUBS * (chips - 1)

    def service(e):
        ev = e // stride

        @pl.when((lax.rem(e, stride) == 0) & (ev < events))
        def _():
            gh.pass_one(1 + ev // SUBS, lax.rem(ev, SUBS))

    attn_grads(blk, qT, kT, vT, dctx, lse, ctx_sum, dqkv_t, k_rows, dk_acc, dv_acc, service)

    def cols_of(d, s):
        return jnp.concatenate([dqkv_t[:, place.span(d, s, own)] for own in (True, False)], axis=1)

    def block(s):
        for d in (0, 1):
            rs.put(d, s, dot(cols_of(d, s).T, w_t[...]))
            if d == 1:
                rs.give(0, s).start()

    def late(d, s):
        gh.arrive(d, s)
        cols = cols_of(d, s)
        dw_out[...] += dot(cols, gh.load(d, s))
        db_out[...] += jnp.sum(cols.astype(F32), axis=1, keepdims=True)

    block(1)
    rs.give(1, 1).start()

    def step(s, _):
        tail = rs.pass_on(s)
        following = lax.rem(s + 1, chips)
        block(following)
        tail.start()
        rs.give(1, following).start()
        ev = done + s - 2

        @pl.when((s >= 2) & (ev < events))
        def _():
            gh.pass_one(1 + ev // SUBS, lax.rem(ev, SUBS))
        for d in (0, 1):
            late(d, s - 1)
        return 0
    lax.fori_loop(1, chips, step, 0)

    vec = jnp.zeros((2, x_in.shape[1]), F32)
    for d in (0, 1):
        rows = slice(d * half, (d + 1) * half)
        x_hat, inv_std, _ = layer_norm_fwd(x_in[rows, :], gain[...], bias[...])
        grad = rs.final(d, rs.own)
        dx_out[rows, :] = (dmid[rows, :].astype(F32) + layer_norm_bwd(grad, x_hat, inv_std, gain[...])).astype(BF16)
        vec += jnp.concatenate([jnp.sum(grad * x_hat, axis=0, keepdims=True), jnp.sum(grad, axis=0, keepdims=True)], axis=0)
    late_part[...] = vec
    vec_out[2:6, :] = first_rows.total()
    last_rows.start()
    for d in (0, 1):
        late(d, chips - 1)
    vec_out[0:2, :] = last_rows.total()
    for one in (g, gh, rs, first_rows, last_rows):
        one.drain()


def attn_stage(n, dmid, ctx_t, ctx_sum, lse, q_t, k_t, v_t, wo, x_in, early, gain, bias, w_t):
    rows, width = x_in.shape
    dim, seq = q_t.shape
    sem = pltpu.SemaphoreType.DMA((n,))
    acc = pltpu.VMEM((dim, seq), F32)
    scratch = gather_scratch(n, rows, width) * 2 + scatter_scratch(n, rows, width) + [
        pltpu.SemaphoreType.DMA, pltpu.VMEM((dim, seq), BF16), pltpu.VMEM((3 * dim, seq), BF16), pltpu.VMEM((seq, dim), BF16), acc, acc,
        pltpu.VMEM((2, width), F32), pltpu.VMEM((n, 4, width), F32), sem, sem, pltpu.VMEM((n, 2, width), F32), sem, sem]
    return comm_call(attn_kernel, n, "attn_stage", 2,
                     (dmid, dmid, ctx_t, ctx_sum, lse, q_t, k_t, v_t, wo, x_in, early, gain, bias, w_t),
                     [((dim, width), F32), ((rows, width), BF16), (w_t.shape, F32), ((3 * dim, 1), F32), ((6, width), F32)], scratch, 63, hbm=(0,))


def solution(mesh):
    def local_backward(x_in, x_mid, d_out, q_saved, k_saved, v_saved, z_saved, ln1_gain, ln1_bias, ln2_gain, ln2_bias, w_qkv, w_proj, w_fc1, w_fc2):
        n = mesh.shape['tp']
        dim = q_saved.shape[-1]
        row = lambda a: a[None, :]
        q_t, k_t, v_t = (jnp.transpose(a[0, :, 0, :]) for a in (q_saved, k_saved, v_saved))
        grad_wfc1, grad_wfc2, grad_bfc1, grad_mid, early, lse, ctx_t, ctx_sum = mlp_stage(
            n, d_out[0], x_mid[0], z_saved[0], row(ln2_gain), row(ln2_bias), w_fc1, w_fc2, q_t, k_t, v_t)
        w_qkv_t = jnp.transpose(w_qkv[:, :, 0, :], (0, 2, 1)).reshape(3 * dim, -1)
        grad_wproj, grad_x, grad_w_t, grad_b, grad_vecs = attn_stage(
            n, grad_mid, ctx_t, ctx_sum, lse, q_t, k_t, v_t, w_proj[0], x_in[0], early, row(ln1_gain), row(ln1_bias), w_qkv_t)
        grad_wqkv = jnp.transpose(grad_w_t.reshape(3, dim, -1), (0, 2, 1))[:, :, None, :]
        return grad_x[None], grad_wqkv, grad_b.reshape(3, 1, dim), grad_wproj[None], grad_wfc1, grad_bfc1[0], grad_wfc2, grad_vecs

    tok_spec = P('dp', 'tp', None)
    head_spec = P('dp', None, 'tp', None)
    in_specs = (tok_spec, tok_spec, tok_spec, head_spec, head_spec, head_spec, P('dp', None, 'tp'),
                P(None), P(None), P(None), P(None),
                P(None, None, 'tp', None), P('tp', None, None), P(None, 'tp'), P('tp', None))
    out_specs = (tok_spec, P('dp', None, 'tp', None), P('dp', 'tp', None), P(('dp', 'tp'), None, None),
                 P('dp', 'tp'), P(('dp', 'tp')), P(('dp', 'tp'), None), P('dp', None))
    return jax.shard_map(local_backward, mesh=mesh, in_specs=in_specs, out_specs=out_specs, check_vma=False)
```

```python
import functools
import jax, jax.numpy as jnp
from jax import lax
from jax.experimental import pallas as pl
from jax.experimental.pallas import tpu as pltpu
from jax.sharding import PartitionSpec as P

F32, BF16 = jnp.float32, jnp.bfloat16
LOG2E = 1.4426950408889634
LN_EPS = 1e-5
GELU_COEF = 0.044715
GELU_SCALE = 0.7978845608028654


def dot(a, b):
    return lax.dot_general(a, b, (((1,), (0,)), ((), ())), preferred_element_type=F32)


def layer_norm_fwd(token_rows, norm_gain, norm_bias):
    rows_f32 = token_rows.astype(jnp.float32)
    centered = rows_f32 - jnp.mean(rows_f32, axis=-1, keepdims=True)
    inv_std = lax.rsqrt(jnp.mean(centered * centered, axis=-1, keepdims=True) + LN_EPS)
    x_hat = centered * inv_std
    return x_hat, inv_std, (x_hat * norm_gain + norm_bias).astype(jnp.bfloat16)


def layer_norm_bwd(grad_norm, x_hat, inv_std, norm_gain):
    grad_hat = grad_norm * norm_gain
    centered_grad = grad_hat - jnp.mean(grad_hat, axis=-1, keepdims=True)
    return inv_std * (centered_grad - x_hat * jnp.mean(grad_hat * x_hat, axis=-1, keepdims=True))


def gelu_parts(pre_act):
    tanh_val = jnp.tanh(GELU_SCALE * (pre_act + GELU_COEF * pre_act * pre_act * pre_act))
    act_value = 0.5 * pre_act * (1.0 + tanh_val)
    act_slope = 0.5 * (1.0 + tanh_val) + 0.5 * pre_act * (1.0 - tanh_val * tanh_val) * GELU_SCALE * (1.0 + 3.0 * GELU_COEF * pre_act * pre_act)
    return act_value, act_slope


def attn_stats(step, blk, qT, kT, vT, k_rows, lse_out, ctx_out, sum_out):
    dim, seq = kT.shape
    c = (dim ** -0.5) * LOG2E
    here = pl.ds(pl.multiple_of(step * blk, blk), blk)
    q = qT[:, here]
    k_rows[here, :] = kT[:, here].T

    def scores(i, masked):
        rows = pl.ds(pl.multiple_of(i * blk, blk), blk)
        s = dot(k_rows[rows, :], q) * c
        if masked:
            r = lax.broadcasted_iota(jnp.int32, (blk, blk), 0)
            col = lax.broadcasted_iota(jnp.int32, (blk, blk), 1)
            s = jnp.where(r <= col, s, -1e30)
        return s

    def stats(i, carry, masked):
        m, l = carry
        s = scores(i, masked)
        new = jnp.maximum(m, jnp.max(s, axis=0, keepdims=True))
        l = l * jnp.exp2(m - new) + jnp.sum(jnp.exp2(s - new), axis=0, keepdims=True)
        return new, l

    init = (jnp.full((1, blk), -1e30, F32), jnp.zeros((1, blk), F32))
    carry = lax.fori_loop(0, step, functools.partial(stats, masked=False), init)
    m, l = stats(step, carry, True)
    lse = m + jnp.log2(l)

    def apply(i, carry, masked):
        low_sum, res_sum = carry
        p = jnp.exp2(scores(i, masked) - lse)
        low = p.astype(BF16)
        res = (p - low.astype(F32)).astype(BF16)
        v = vT[:, pl.ds(pl.multiple_of(i * blk, blk), blk)]
        return low_sum + dot(v, low), res_sum + dot(v, res)

    zero = jnp.zeros((dim, blk), F32)
    carry = lax.fori_loop(0, step, functools.partial(apply, masked=False), (zero, zero))
    low_sum, res_sum = apply(step, carry, True)
    ctx_out[:, here] = low_sum.astype(BF16)
    sum_out[:, here] = low_sum + res_sum
    lse_out[:, here] = jnp.broadcast_to(lse, (8, blk))


def attn_grads(blk, qT, kT, vT, dctxT, lse, ctxsum, out, k_rows, dk_acc, dv_acc, service):
    dim, seq = kT.shape
    scale = dim ** -0.5
    c = scale * LOG2E

    def queries(step, _):
        here = pl.ds(pl.multiple_of(step * blk, blk), blk)
        qt = qT[:, here]
        dct = dctxT[:, here]
        q = qt.T
        dc = dct.T
        delta_row = jnp.sum(dct.astype(F32) * ctxsum[:, here], axis=0, keepdims=True)
        lse_col = jnp.broadcast_to(lse[0:1, here], (128, blk)).T[:, :1]
        delta_col = jnp.broadcast_to(delta_row, (128, blk)).T[:, :1]
        base = step * (step + 1) // 2

        def block(i, dq, masked):
            service(base + i)
            cols = pl.ds(pl.multiple_of(i * blk, blk), blk)
            s = dot(q, kT[:, cols]) * c
            dp = dot(dc, vT[:, cols])
            p = jnp.exp2(s - lse_col)
            if masked:
                r = lax.broadcasted_iota(jnp.int32, (blk, blk), 0)
                col = lax.broadcasted_iota(jnp.int32, (blk, blk), 1)
                p = jnp.where(r >= col, p, 0.0)
            ds = (p * (dp - delta_col)).astype(BF16)
            dv_acc[:, cols] += dot(dct, p.astype(BF16))
            dk_acc[:, cols] += dot(qt, ds)
            return dq + dot(ds, k_rows[cols, :])

        dq = lax.fori_loop(0, step, functools.partial(block, masked=False), jnp.zeros((blk, dim), F32))
        dq = block(step, dq, True)
        out[0:dim, here] = (dq * scale).T.astype(BF16)
        return 0
    lax.fori_loop(0, seq // blk, queries, 0)

    def put(i, _):
        cols = pl.ds(pl.multiple_of(i * blk, blk), blk)
        out[dim:2 * dim, cols] = (dk_acc[:, cols] * scale).astype(BF16)
        out[2 * dim:3 * dim, cols] = dv_acc[:, cols].astype(BF16)
        return 0
    lax.fori_loop(0, seq // blk, put, 0)


MESH = pl.DeviceIdType.MESH
SUBS = 2


def dot_nt(a, b):
    return lax.dot_general(a, b, (((1,), (1,)), ((), ())), preferred_element_type=F32)


def remote(src, dst, send_sem, recv_sem, dev):
    return pltpu.make_async_remote_copy(src_ref=src, dst_ref=dst, send_sem=send_sem, recv_sem=recv_sem,
                                        device_id={'tp': dev}, device_id_type=MESH)


class Place:
    def __init__(self, n, rows):
        me = lax.axis_index('tp')
        self.me, self.n, self.chips, self.half, self.rows = me, n, n // 2, rows // 2, rows
        self.core, self.chip = lax.rem(me, 2), me // 2
        self.partner = me + 1 - 2 * self.core
        self.next = (lax.rem(me + 2, n), lax.rem(me + n - 2, n))
        self.sub = self.half // SUBS

    def origin(self, d, s):
        return lax.rem(self.chip + (self.chips - s if d == 0 else s), self.chips)

    def span(self, d, s, own):
        core = self.core if own else 1 - self.core
        start = (2 * self.origin(d, s) + core) * self.rows + d * self.half
        return pl.ds(pl.multiple_of(start, self.half), self.half)

    def part(self, d, s, own, sub):
        core = self.core if own else 1 - self.core
        start = (2 * self.origin(d, s) + core) * self.rows + d * self.half + sub * self.sub
        return pl.ds(pl.multiple_of(start, self.sub), self.sub)

    def greet(self):
        barrier = pltpu.get_barrier_semaphore()
        for dev in (self.next[0], self.next[1], self.partner):
            pl.semaphore_signal(barrier, inc=1, device_id={'tp': dev}, device_id_type=MESH)
        pl.semaphore_wait(barrier, 3)

    def greet_all(self):
        barrier = pltpu.get_barrier_semaphore()

        def hello(r, _):
            pl.semaphore_signal(barrier, inc=1, device_id={'tp': lax.rem(self.me + r, self.n)}, device_id_type=MESH)
            return 0
        lax.fori_loop(1, self.n, hello, 0)
        pl.semaphore_wait(barrier, self.n - 1)


class Gather:
    def __init__(self, place, buf, send, recv, psend, precv):
        self.p, self.buf, self.send, self.recv, self.psend, self.precv = place, buf, send, recv, psend, precv

    def hop(self, d, s, sub):
        at = self.buf.at[self.p.part(d, s, True, sub)]
        return remote(at, at, self.send.at[d, s, sub], self.recv.at[d, s, sub], self.p.next[d])

    def give(self, d, s, sub):
        at = self.buf.at[self.p.part(d, s, True, sub)]
        return remote(at, at, self.psend.at[d, s, sub], self.precv.at[d, s, sub], self.p.partner)

    def first_way(self, d):
        for sub in range(SUBS):
            self.hop(d, 0, sub).start()
            self.give(d, 0, sub).start()

    def first(self):
        for sub in range(SUBS):
            for d in (0, 1):
                self.hop(d, 0, sub).start()
        for sub in range(SUBS):
            for d in (0, 1):
                self.give(d, 0, sub).start()

    def pass_one(self, s, sub):
        for d in (0, 1):
            at = self.buf.at[self.p.part(d, s, True, sub)]
            remote(at, at, self.send.at[d, s - 1, sub], self.recv.at[d, s - 1, sub], self.p.next[d]).wait_recv()

            @pl.when(s < self.p.chips - 1)
            def _():
                self.hop(d, s, sub).start()
            self.give(d, s, sub).start()

    def pass_on(self, s):
        for sub in range(SUBS):
            self.pass_one(s, sub)

    def arrive(self, d, s):
        for sub in range(SUBS):
            at = self.buf.at[self.p.part(d, s, False, sub)]
            remote(at, at, self.psend.at[d, s, sub], self.precv.at[d, s, sub], self.p.partner).wait_recv()

    def load(self, d, s):
        return jnp.concatenate([self.buf[self.p.span(d, s, True), :], self.buf[self.p.span(d, s, False), :]], axis=0)

    def drain(self):
        def one(s, _):
            for d in (0, 1):
                for sub in range(SUBS):
                    self.give(d, s, sub).wait_send()

                    @pl.when(s < self.p.chips - 1)
                    def _():
                        self.hop(d, s, sub).wait_send()
            return 0
        lax.fori_loop(0, self.p.chips, one, 0)


class Scatter:
    def __init__(self, place, own, keep, out, inc, pout, pinc, send, recv, psend, precv):
        self.p, self.own, self.keep, self.out, self.inc, self.send, self.recv = place, own, keep, out, inc, send, recv
        self.pout, self.pinc, self.psend, self.precv = pout, pinc, psend, precv

    def give(self, d, s):
        return remote(self.pout.at[d, s], self.pinc.at[d, s], self.psend.at[d, s], self.precv.at[d, s], self.p.partner)

    def hop(self, d, r, sub):
        rows = slice(sub * self.p.sub, (sub + 1) * self.p.sub)
        return remote(self.out.at[d, r, rows], self.inc.at[d, r, rows], self.send.at[d, r, sub], self.recv.at[d, r, sub], self.p.next[d])

    def put(self, d, s, part, first=False):
        half = self.p.half
        (self.keep if first else self.own)[d] = part[:half]
        self.pout[d, s] = part[half:].astype(BF16)

    def join(self, d, s):
        self.give(d, s).wait_recv()
        self.own[d] += self.pinc[d, s].astype(F32)

    def forward(self, d, s, sub):
        rows = slice(sub * self.p.sub, (sub + 1) * self.p.sub)

        @pl.when(s >= 2)
        def _():
            self.hop(d, s - 2, sub).wait_recv()
            self.out[d, s - 1, rows] = (self.own[d, rows] + self.inc[d, s - 2, rows].astype(F32)).astype(BF16)

        @pl.when(s < 2)
        def _():
            self.out[d, s - 1, rows] = self.own[d, rows].astype(BF16)

    def pass_on(self, s):
        for d in (0, 1):
            self.join(d, s)
        before = None
        for sub in range(SUBS):
            for d in (0, 1):
                self.forward(d, s, sub)
                if before is not None:
                    self.hop(*before).start()
                before = (d, s - 1, sub)
        return self.hop(*before)

    def final(self, d, store):
        last = self.p.chips - 2
        self.give(d, 0).wait_recv()
        for sub in range(SUBS):
            self.hop(d, last, sub).wait_recv()
        return store[d] + self.pinc[d, 0].astype(F32) + self.inc[d, last].astype(F32)

    def drain(self):
        def one(s, _):
            for d in (0, 1):
                self.give(d, s).wait_send()
                for sub in range(SUBS):
                    @pl.when(s < self.p.chips - 1)
                    def _():
                        self.hop(d, s, sub).wait_send()
            return 0
        lax.fori_loop(0, self.p.chips, one, 0)


def gather_sems(n):
    return [pltpu.SemaphoreType.DMA((2, n // 2, SUBS))] * 4


def scatter_sems(n):
    sem = pltpu.SemaphoreType.DMA((2, n // 2))
    fine = pltpu.SemaphoreType.DMA((2, n // 2, SUBS))
    return [fine, fine, sem, sem]


def scatter_bufs(n, rows, width):
    chips, half = n // 2, rows // 2
    wide = pltpu.VMEM((2, half, width), F32)
    ring = pltpu.VMEM((2, chips - 1, half, width), BF16)
    pair = pltpu.VMEM((2, chips, half, width), BF16)
    return [wide, wide, ring, ring, pair, pair]


class Spread:
    def __init__(self, place, part, buf, send, recv):
        self.p, self.part, self.buf, self.send, self.recv = place, part, buf, send, recv

    def to(self, r):
        me = self.p.me
        return remote(self.part, self.buf.at[me], self.send.at[r], self.recv.at[me], lax.rem(me + r, self.p.n))

    def start(self):
        def one(r, _):
            self.to(r).start()
            return 0
        lax.fori_loop(1, self.p.n, one, 0)
        self.buf[pl.ds(self.p.me, 1)] = self.part[...][None]

    def total(self):
        def one(r, _):
            src = lax.rem(self.p.me + self.p.n - r, self.p.n)
            remote(self.part, self.buf.at[src], self.send.at[r], self.recv.at[src], src).wait_recv()
            return 0
        lax.fori_loop(1, self.p.n, one, 0)
        return lax.fori_loop(1, self.p.n, lambda j, acc: acc + self.buf[j], self.buf[0])

    def drain(self):
        def one(r, _):
            self.to(r).wait_send()
            return 0
        lax.fori_loop(1, self.p.n, one, 0)


def layer_kernel(n, loads, *refs):
    hbm, refs = refs[:loads], refs[loads:]
    gain2, bias2, gain1, bias1, dw1_out, dw2_out, db1_out, dwo_out, dx_out, dw_out, db_out, vec_out = refs[:12]
    x_mid, z, w1, w2, qT, kT, vT, wo, x_in, w_t = refs[12:12 + loads - 1]
    scratch = refs[12 + loads - 1:]
    load_sems, gy_buf, gh_buf = scratch[:3]
    rs_bufs, gathers, scatters, rest = scratch[3:9], scratch[9:25], scratch[25:33], scratch[33:]
    w1_t, w2_t, dw1_t, k_rows, lse, ctx_t, ctx_sum, dctx, dqkv_t, dk_acc, dv_acc, early, late_part, e_buf, e_send, e_recv, l_buf, l_send, l_recv = rest
    rows_here, width = x_mid.shape
    place = Place(n, rows_here)
    half, chips = place.half, place.chips
    seq = kT.shape[1]
    blk = seq // chips
    gy, gh, gm, g1 = (Gather(place, buf, *gathers[4 * i:4 * i + 4]) for i, buf in enumerate((gy_buf, gh_buf, gy_buf, gh_buf)))
    rs2, rs1 = (Scatter(place, *rs_bufs, *scatters[4 * i:4 * i + 4]) for i in range(2))
    first_rows, last_rows = Spread(place, early, e_buf, e_send, e_recv), Spread(place, late_part, l_buf, l_send, l_recv)
    mine = pl.ds(pl.multiple_of(place.me * rows_here, rows_here), rows_here)
    way = [pl.ds(pl.multiple_of(place.me * rows_here + d * half, half), half) for d in (0, 1)]

    copies = [pltpu.make_async_copy(hbm[0], gy_buf.at[mine], load_sems.at[0])]
    copies += [pltpu.make_async_copy(hbm[i], refs[11 + i], load_sems.at[i]) for i in range(1, loads)]
    for c in copies:
        c.start()
    place.greet_all()
    copies[0].wait()
    gy.first()
    for c in copies[1:]:
        c.wait()
    gh_buf[mine, :] = layer_norm_fwd(x_mid[...], gain2[...], bias2[...])[2]
    w1_t[...] = w1[...].T
    w2_t[...] = w2[...].T
    for acc in (dw1_t, dw2_out, db1_out, dwo_out, dw_out, db_out, dk_acc, dv_acc):
        acc[...] = jnp.zeros_like(acc)
    gh.first()

    def block(d, s, first):
        gy.arrive(d, s)
        dy = gy.load(d, s)
        pre = jnp.concatenate([z[place.span(d, s, True), :], z[place.span(d, s, False), :]], axis=0).astype(F32)
        act, slope = gelu_parts(pre)
        dz = (dot(dy, w2_t[...]) * slope).astype(BF16)
        rs2.put(d, s, dot(dz, w1_t[...]), first)
        if d == 1:
            rs2.give(0, s).start()
        dw2_out[...] += dot(act.astype(BF16).T, dy)
        db1_out[...] += jnp.sum(dz.astype(F32), axis=0, keepdims=True)
        return dz

    def late(d, s, dz):
        gh.arrive(d, s)
        dw1_t[...] += dot(dz.T, gh.load(d, s))

    def attend(s):
        attn_stats(s, blk, qT, kT, vT, k_rows, lse, ctx_t, ctx_sum)

    dz = [block(d, 0, True) for d in (0, 1)]
    rs2.give(1, 0).start()
    for d in (0, 1):
        late(d, 0, dz[d])
    attend(0)

    def mlp_step(s, _):
        gy.pass_on(s)
        dz = [block(d, s, False) for d in (0, 1)]

        @pl.when(s == chips - 1)
        def _():
            gy.drain()
        rs2.give(1, s).start()
        tail = rs2.pass_on(s)
        gh.pass_on(s)
        tail.start()
        for d in (0, 1):
            late(d, s, dz[d])
        attend(s)
        return 0
    lax.fori_loop(1, chips, mlp_step, 0)
    gh.drain()

    for d in (0, 1):
        rs2.own[d] = rs2.final(d, rs2.keep)
    vec = jnp.zeros((4, width), F32)
    for d in (0, 1):
        rows = slice(d * half, (d + 1) * half)
        x_hat, inv_std, _ = layer_norm_fwd(x_mid[rows, :], gain2[...], bias2[...])
        grad = rs2.own[d]
        dy = gy_buf[way[d], :].astype(F32)
        dmid = (dy + layer_norm_bwd(grad, x_hat, inv_std, gain2[...])).astype(BF16)
        gy_buf[way[d], :] = dmid
        vec += jnp.concatenate([jnp.sum(a, axis=0, keepdims=True) for a in (grad * x_hat, grad, dmid.astype(F32), dy)], axis=0)
        gm.first_way(d)
    early[...] = vec
    rs2.drain()
    gh_buf[mine, :] = layer_norm_fwd(x_in[...], gain1[...], bias1[...])[2]

    def project(d, s):
        gm.arrive(d, s)
        rows = gm.load(d, s)
        both = dot_nt(wo[...], rows).astype(BF16)
        cols = [place.span(d, s, own) for own in (True, False)]
        dctx[:, cols[0]] = both[:, :half]
        dctx[:, cols[1]] = both[:, half:]
        dwo_out[...] += dot(jnp.concatenate([ctx_t[:, c] for c in cols], axis=1), rows)

    for d in (0, 1):
        project(d, 0)
    dw1_out[...] = dw1_t[...].T

    def mid_step(s, _):
        gm.pass_on(s)
        for d in (0, 1):
            project(d, s)
        return 0
    lax.fori_loop(1, chips - 1, mid_step, 0)
    gm.pass_on(chips - 1)
    g1.first()
    first_rows.start()
    for d in (0, 1):
        project(d, chips - 1)

    stride = 3
    blocks = chips * (chips + 1) // 2
    events = SUBS * (chips - 1)
    left = list(range((blocks + stride - 1) // stride, events))

    def event(ev):
        g1.pass_one(1 + ev // SUBS, ev % SUBS if isinstance(ev, int) else lax.rem(ev, SUBS))

    def service(e):
        ev = e // stride

        @pl.when((lax.rem(e, stride) == 0) & (ev < events))
        def _():
            event(ev)

    attn_grads(blk, qT, kT, vT, dctx, lse, ctx_sum, dqkv_t, k_rows, dk_acc, dv_acc, service)

    def cols_of(d, s):
        return jnp.concatenate([dqkv_t[:, place.span(d, s, own)] for own in (True, False)], axis=1)

    def back(s):
        for d in (0, 1):
            rows = cols_of(d, s).T
            rs1.put(d, s, dot(rows, w_t[...]))
            if d == 1:
                rs1.give(0, s).start()
            db_out[...] += jnp.sum(rows.astype(F32), axis=0, keepdims=True)

    def weigh(d, s):
        g1.arrive(d, s)
        dw_out[...] += dot(cols_of(d, s), g1.load(d, s))

    for ev in left[:1]:
        event(ev)
    back(1)
    rs1.give(1, 1).start()
    for ev in left[1:]:
        event(ev)

    def qkv_step(s, _):
        tail = rs1.pass_on(s)
        following = lax.rem(s + 1, chips)
        back(following)
        tail.start()
        rs1.give(1, following).start()
        for d in (0, 1):
            weigh(d, s - 1)
        return 0
    lax.fori_loop(1, chips, qkv_step, 0)

    vec = jnp.zeros((2, width), F32)
    for d in (0, 1):
        rows = slice(d * half, (d + 1) * half)
        x_hat, inv_std, _ = layer_norm_fwd(x_in[rows, :], gain1[...], bias1[...])
        grad = rs1.final(d, rs1.own)
        dx_out[rows, :] = (gy_buf[way[d], :].astype(F32) + layer_norm_bwd(grad, x_hat, inv_std, gain1[...])).astype(BF16)
        vec += jnp.concatenate([jnp.sum(grad * x_hat, axis=0, keepdims=True), jnp.sum(grad, axis=0, keepdims=True)], axis=0)
    late_part[...] = vec
    vec_out[2:6, :] = first_rows.total()
    last_rows.start()
    for d in (0, 1):
        weigh(d, chips - 1)
    vec_out[0:2, :] = last_rows.total()
    for one in (gm, g1, rs1, first_rows, last_rows):
        one.drain()


def layer_stage(n, dout, x_mid, z, w1, w2, q_t, k_t, v_t, wo, x_in, w_t, gain2, bias2, gain1, bias1):
    rows, width = dout.shape
    units = z.shape[1]
    dim, seq = q_t.shape
    hbm = (dout, x_mid, z, w1, w2, q_t, k_t, v_t, wo, x_in, w_t)
    vm = pl.BlockSpec(memory_space=pltpu.VMEM)
    full = pltpu.VMEM((n * rows, width), BF16)
    sem = pltpu.SemaphoreType.DMA((n,))
    acc = pltpu.VMEM((dim, seq), F32)
    scratch = [pltpu.VMEM(a.shape, a.dtype) for a in hbm[1:]] + [pltpu.SemaphoreType.DMA((len(hbm),)), full, full]
    scratch += scatter_bufs(n, rows, width) + gather_sems(n) * 4 + scatter_sems(n) * 2
    scratch += [pltpu.VMEM((units, width), BF16), pltpu.VMEM((width, units), BF16), pltpu.VMEM((units, width), F32),
                pltpu.VMEM((seq, dim), BF16), pltpu.VMEM((8, seq), F32), pltpu.VMEM((dim, seq), BF16), acc,
                pltpu.VMEM((dim, seq), BF16), pltpu.VMEM((3 * dim, seq), BF16), acc, acc,
                pltpu.VMEM((4, width), F32), pltpu.VMEM((2, width), F32),
                pltpu.VMEM((n, 4, width), F32), sem, sem, pltpu.VMEM((n, 2, width), F32), sem, sem]
    outs = [((width, units), F32), ((units, width), F32), ((1, units), F32), ((dim, width), F32), ((rows, width), BF16),
            (w_t.shape, F32), ((1, 3 * dim), F32), ((6, width), F32)]
    return pl.pallas_call(
        functools.partial(layer_kernel, n, len(hbm)),
        in_specs=[pl.BlockSpec(memory_space=pl.ANY)] * len(hbm) + [vm] * 4,
        out_specs=[vm] * len(outs),
        out_shape=[jax.ShapeDtypeStruct(*o) for o in outs],
        scratch_shapes=scratch,
        compiler_params=pltpu.CompilerParams(collective_id=1, has_side_effects=True, vmem_limit_bytes=67043328),
        name="layer_stage",
    )(*hbm, gain2, bias2, gain1, bias1)


def deliver_kernel(count, *refs):
    for i in range(count):
        refs[count + i][...] = refs[i][...]


def deliver(big, small, steps=4):
    cut = [pl.BlockSpec((a.shape[0] // steps, a.shape[1]), lambda i: (i, 0)) for a in big]
    whole = [pl.BlockSpec(a.shape, lambda i: (0, 0)) for a in small]
    args = list(big) + list(small)
    return pl.pallas_call(
        functools.partial(deliver_kernel, len(args)),
        grid=(steps,),
        in_specs=cut + whole,
        out_specs=cut + whole,
        out_shape=[jax.ShapeDtypeStruct(a.shape, a.dtype) for a in args],
        compiler_params=pltpu.CompilerParams(dimension_semantics=("arbitrary",), vmem_limit_bytes=67043328),
        name="deliver",
    )(*args)


def solution(mesh):
    def local_backward(x_in, x_mid, d_out, q_saved, k_saved, v_saved, z_saved, ln1_gain, ln1_bias, ln2_gain, ln2_bias, w_qkv, w_proj, w_fc1, w_fc2):
        n = mesh.shape['tp']
        dim = q_saved.shape[-1]
        row = lambda a: a[None, :]
        q_t, k_t, v_t = (jnp.transpose(a[0, :, 0, :]) for a in (q_saved, k_saved, v_saved))
        w_qkv_t = jnp.transpose(w_qkv[:, :, 0, :], (0, 2, 1)).reshape(3 * dim, -1)
        dw1, dw2, db1, dwo, dx, dw_t, db, vecs = layer_stage(
            n, d_out[0], x_mid[0], z_saved[0], w_fc1, w_fc2, q_t, k_t, v_t, w_proj[0], x_in[0], w_qkv_t,
            row(ln2_gain), row(ln2_bias), row(ln1_gain), row(ln1_bias))
        dx, dw_t, dwo, dw1, dw2, db1, db, vecs = deliver((dx, dw_t, dwo, dw1, dw2), (db1, db, vecs))
        grad_wqkv = jnp.transpose(dw_t.reshape(3, dim, -1), (0, 2, 1))[:, :, None, :]
        return dx[None], grad_wqkv, db.reshape(3, 1, dim), dwo[None], dw1, db1[0], dw2, vecs

    tok_spec = P('dp', 'tp', None)
    head_spec = P('dp', None, 'tp', None)
    in_specs = (tok_spec, tok_spec, tok_spec, head_spec, head_spec, head_spec, P('dp', None, 'tp'),
                P(None), P(None), P(None), P(None),
                P(None, None, 'tp', None), P('tp', None, None), P(None, 'tp'), P('tp', None))
    out_specs = (tok_spec, P('dp', None, 'tp', None), P('dp', 'tp', None), P(('dp', 'tp'), None, None),
                 P('dp', 'tp'), P(('dp', 'tp')), P(('dp', 'tp'), None), P('dp', None))
    return jax.shard_map(local_backward, mesh=mesh, in_specs=in_specs, out_specs=out_specs, check_vma=False)
```

```python
import functools
import jax, jax.numpy as jnp
from jax import lax
from jax.experimental import pallas as pl
from jax.experimental.pallas import tpu as pltpu
from jax.sharding import PartitionSpec as P

F32, BF16 = jnp.float32, jnp.bfloat16
LOG2E = 1.4426950408889634
LN_EPS = 1e-5
GELU_COEF = 0.044715
GELU_SCALE = 0.7978845608028654


def dot(a, b):
    return lax.dot_general(a, b, (((1,), (0,)), ((), ())), preferred_element_type=F32)


def layer_norm_fwd(token_rows, norm_gain, norm_bias):
    rows_f32 = token_rows.astype(jnp.float32)
    centered = rows_f32 - jnp.mean(rows_f32, axis=-1, keepdims=True)
    inv_std = lax.rsqrt(jnp.mean(centered * centered, axis=-1, keepdims=True) + LN_EPS)
    x_hat = centered * inv_std
    return x_hat, inv_std, (x_hat * norm_gain + norm_bias).astype(jnp.bfloat16)


def layer_norm_bwd(grad_norm, x_hat, inv_std, norm_gain):
    grad_hat = grad_norm * norm_gain
    centered_grad = grad_hat - jnp.mean(grad_hat, axis=-1, keepdims=True)
    return inv_std * (centered_grad - x_hat * jnp.mean(grad_hat * x_hat, axis=-1, keepdims=True))


def gelu_parts(pre_act):
    tanh_val = jnp.tanh(GELU_SCALE * (pre_act + GELU_COEF * pre_act * pre_act * pre_act))
    act_value = 0.5 * pre_act * (1.0 + tanh_val)
    act_slope = 0.5 * (1.0 + tanh_val) + 0.5 * pre_act * (1.0 - tanh_val * tanh_val) * GELU_SCALE * (1.0 + 3.0 * GELU_COEF * pre_act * pre_act)
    return act_value, act_slope


def attn_stats(step, blk, qT, kT, vT, k_rows, lse_out, ctx_out, sum_out):
    dim, seq = kT.shape
    c = (dim ** -0.5) * LOG2E
    here = pl.ds(pl.multiple_of(step * blk, blk), blk)
    q = qT[:, here]
    k_rows[here, :] = kT[:, here].T

    def scores(i, masked):
        rows = pl.ds(pl.multiple_of(i * blk, blk), blk)
        s = dot(k_rows[rows, :], q) * c
        if masked:
            r = lax.broadcasted_iota(jnp.int32, (blk, blk), 0)
            col = lax.broadcasted_iota(jnp.int32, (blk, blk), 1)
            s = jnp.where(r <= col, s, -1e30)
        return s

    def stats(i, carry, masked):
        m, l = carry
        s = scores(i, masked)
        new = jnp.maximum(m, jnp.max(s, axis=0, keepdims=True))
        l = l * jnp.exp2(m - new) + jnp.sum(jnp.exp2(s - new), axis=0, keepdims=True)
        return new, l

    init = (jnp.full((1, blk), -1e30, F32), jnp.zeros((1, blk), F32))
    carry = lax.fori_loop(0, step, functools.partial(stats, masked=False), init)
    m, l = stats(step, carry, True)
    lse = m + jnp.log2(l)

    def apply(i, carry, masked):
        low_sum, res_sum = carry
        p = jnp.exp2(scores(i, masked) - lse)
        low = p.astype(BF16)
        res = (p - low.astype(F32)).astype(BF16)
        v = vT[:, pl.ds(pl.multiple_of(i * blk, blk), blk)]
        return low_sum + dot(v, low), res_sum + dot(v, res)

    zero = jnp.zeros((dim, blk), F32)
    carry = lax.fori_loop(0, step, functools.partial(apply, masked=False), (zero, zero))
    low_sum, res_sum = apply(step, carry, True)
    ctx_out[:, here] = low_sum.astype(BF16)
    sum_out[:, here] = low_sum + res_sum
    lse_out[:, here] = jnp.broadcast_to(lse, (8, blk))


def attn_grads(blk, qT, kT, vT, dctxT, lse, ctxsum, out, k_rows, dk_acc, dv_acc, service):
    dim, seq = kT.shape
    scale = dim ** -0.5
    c = scale * LOG2E

    def queries(step, _):
        here = pl.ds(pl.multiple_of(step * blk, blk), blk)
        qt = qT[:, here]
        dct = dctxT[:, here]
        q = qt.T
        dc = dct.T
        delta_row = jnp.sum(dct.astype(F32) * ctxsum[:, here], axis=0, keepdims=True)
        lse_col = jnp.broadcast_to(lse[0:1, here], (128, blk)).T[:, :1]
        delta_col = jnp.broadcast_to(delta_row, (128, blk)).T[:, :1]
        base = step * (step + 1) // 2

        def block(i, dq, masked):
            service(base + i)
            cols = pl.ds(pl.multiple_of(i * blk, blk), blk)
            s = dot(q, kT[:, cols]) * c
            dp = dot(dc, vT[:, cols])
            p = jnp.exp2(s - lse_col)
            if masked:
                r = lax.broadcasted_iota(jnp.int32, (blk, blk), 0)
                col = lax.broadcasted_iota(jnp.int32, (blk, blk), 1)
                p = jnp.where(r >= col, p, 0.0)
            ds = (p * (dp - delta_col)).astype(BF16)
            dv_acc[:, cols] += dot(dct, p.astype(BF16))
            dk_acc[:, cols] += dot(qt, ds)
            return dq + dot(ds, k_rows[cols, :])

        dq = lax.fori_loop(0, step, functools.partial(block, masked=False), jnp.zeros((blk, dim), F32))
        dq = block(step, dq, True)
        out[0:dim, here] = (dq * scale).T.astype(BF16)
        return 0
    lax.fori_loop(0, seq // blk, queries, 0)

    def put(i, _):
        cols = pl.ds(pl.multiple_of(i * blk, blk), blk)
        out[dim:2 * dim, cols] = (dk_acc[:, cols] * scale).astype(BF16)
        out[2 * dim:3 * dim, cols] = dv_acc[:, cols].astype(BF16)
        return 0
    lax.fori_loop(0, seq // blk, put, 0)


MESH = pl.DeviceIdType.MESH
SUBS = 2


def dot_nt(a, b):
    return lax.dot_general(a, b, (((1,), (1,)), ((), ())), preferred_element_type=F32)


def remote(src, dst, send_sem, recv_sem, dev):
    return pltpu.make_async_remote_copy(src_ref=src, dst_ref=dst, send_sem=send_sem, recv_sem=recv_sem,
                                        device_id={'tp': dev}, device_id_type=MESH)


class Place:
    def __init__(self, n, rows):
        me = lax.axis_index('tp')
        self.me, self.n, self.chips, self.half, self.rows = me, n, n // 2, rows // 2, rows
        self.core, self.chip = lax.rem(me, 2), me // 2
        self.partner = me + 1 - 2 * self.core
        self.next = (lax.rem(me + 2, n), lax.rem(me + n - 2, n))

    def origin(self, d, s):
        return lax.rem(self.chip + (self.chips - s if d == 0 else s), self.chips)

    def span(self, d, s, own):
        core = self.core if own else 1 - self.core
        start = (2 * self.origin(d, s) + core) * self.rows + d * self.half
        return pl.ds(pl.multiple_of(start, self.half), self.half)

    def part(self, d, s, own, sub, subs):
        core, size = self.core if own else 1 - self.core, self.half // subs
        start = (2 * self.origin(d, s) + core) * self.rows + d * self.half + sub * size
        return pl.ds(pl.multiple_of(start, size), size)

    def greet(self):
        barrier = pltpu.get_barrier_semaphore()
        for dev in (self.next[0], self.next[1], self.partner):
            pl.semaphore_signal(barrier, inc=1, device_id={'tp': dev}, device_id_type=MESH)
        pl.semaphore_wait(barrier, 3)

    def greet_all(self):
        barrier = pltpu.get_barrier_semaphore()

        def hello(r, _):
            pl.semaphore_signal(barrier, inc=1, device_id={'tp': lax.rem(self.me + r, self.n)}, device_id_type=MESH)
            return 0
        lax.fori_loop(1, self.n, hello, 0)
        pl.semaphore_wait(barrier, self.n - 1)


class Gather:
    def __init__(self, subs, place, buf, send, recv, psend, precv):
        self.subs, self.p, self.buf, self.send, self.recv, self.psend, self.precv = subs, place, buf, send, recv, psend, precv

    def hop(self, d, s, sub):
        at = self.buf.at[self.p.part(d, s, True, sub, self.subs)]
        return remote(at, at, self.send.at[d, s, sub], self.recv.at[d, s, sub], self.p.next[d])

    def give(self, d, s, sub):
        at = self.buf.at[self.p.part(d, s, True, sub, self.subs)]
        return remote(at, at, self.psend.at[d, s, sub], self.precv.at[d, s, sub], self.p.partner)

    def first_way(self, d):
        for sub in range(self.subs):
            self.hop(d, 0, sub).start()
            self.give(d, 0, sub).start()

    def first(self):
        for sub in range(self.subs):
            for d in (0, 1):
                self.hop(d, 0, sub).start()
        for sub in range(self.subs):
            for d in (0, 1):
                self.give(d, 0, sub).start()

    def pass_one(self, s, sub):
        for d in (0, 1):
            at = self.buf.at[self.p.part(d, s, True, sub, self.subs)]
            remote(at, at, self.send.at[d, s - 1, sub], self.recv.at[d, s - 1, sub], self.p.next[d]).wait_recv()

            @pl.when(s < self.p.chips - 1)
            def _():
                self.hop(d, s, sub).start()
            self.give(d, s, sub).start()

    def pass_on(self, s):
        for sub in range(self.subs):
            self.pass_one(s, sub)

    def arrive(self, d, s):
        for sub in range(self.subs):
            at = self.buf.at[self.p.part(d, s, False, sub, self.subs)]
            remote(at, at, self.psend.at[d, s, sub], self.precv.at[d, s, sub], self.p.partner).wait_recv()

    def load(self, d, s):
        return jnp.concatenate([self.buf[self.p.span(d, s, True), :], self.buf[self.p.span(d, s, False), :]], axis=0)

    def drain(self):
        def one(s, _):
            for d in (0, 1):
                for sub in range(self.subs):
                    self.give(d, s, sub).wait_send()

                    @pl.when(s < self.p.chips - 1)
                    def _():
                        self.hop(d, s, sub).wait_send()
            return 0
        lax.fori_loop(0, self.p.chips, one, 0)


class Scatter:
    def __init__(self, subs, place, own, keep, out, inc, pout, pinc, send, recv, psend, precv):
        self.subs, self.size = subs, place.half // subs
        self.p, self.own, self.keep, self.out, self.inc, self.send, self.recv = place, own, keep, out, inc, send, recv
        self.pout, self.pinc, self.psend, self.precv = pout, pinc, psend, precv

    def give(self, d, s):
        return remote(self.pout.at[d, s], self.pinc.at[d, s], self.psend.at[d, s], self.precv.at[d, s], self.p.partner)

    def hop(self, d, r, sub):
        rows = slice(sub * self.size, (sub + 1) * self.size)
        return remote(self.out.at[d, r, rows], self.inc.at[d, r, rows], self.send.at[d, r, sub], self.recv.at[d, r, sub], self.p.next[d])

    def put(self, d, s, part, first=False):
        half = self.p.half
        (self.keep if first else self.own)[d] = part[:half]
        self.pout[d, s] = part[half:].astype(BF16)

    def join(self, d, s):
        self.give(d, s).wait_recv()
        self.own[d] += self.pinc[d, s].astype(F32)

    def forward(self, d, s, sub):
        rows = slice(sub * self.size, (sub + 1) * self.size)

        @pl.when(s >= 2)
        def _():
            self.hop(d, s - 2, sub).wait_recv()
            self.out[d, s - 1, rows] = (self.own[d, rows] + self.inc[d, s - 2, rows].astype(F32)).astype(BF16)

        @pl.when(s < 2)
        def _():
            self.out[d, s - 1, rows] = self.own[d, rows].astype(BF16)

    def pass_on(self, s):
        for d in (0, 1):
            self.join(d, s)
        before = None
        for sub in range(self.subs):
            for d in (0, 1):
                self.forward(d, s, sub)
                if before is not None:
                    self.hop(*before).start()
                before = (d, s - 1, sub)
        return self.hop(*before)

    def final(self, d, store):
        last = self.p.chips - 2
        self.give(d, 0).wait_recv()
        for sub in range(self.subs):
            self.hop(d, last, sub).wait_recv()
        return store[d] + self.pinc[d, 0].astype(F32) + self.inc[d, last].astype(F32)

    def drain(self):
        def one(s, _):
            for d in (0, 1):
                self.give(d, s).wait_send()
                for sub in range(self.subs):
                    @pl.when(s < self.p.chips - 1)
                    def _():
                        self.hop(d, s, sub).wait_send()
            return 0
        lax.fori_loop(0, self.p.chips, one, 0)


def gather_sems(n):
    return [pltpu.SemaphoreType.DMA((2, n // 2, SUBS))] * 4


def scatter_sems(n):
    sem = pltpu.SemaphoreType.DMA((2, n // 2))
    fine = pltpu.SemaphoreType.DMA((2, n // 2, SUBS))
    return [fine, fine, sem, sem]


def scatter_bufs(n, rows, width):
    chips, half = n // 2, rows // 2
    wide = pltpu.VMEM((2, half, width), F32)
    ring = pltpu.VMEM((2, chips - 1, half, width), BF16)
    pair = pltpu.VMEM((2, chips, half, width), BF16)
    return [wide, wide, ring, ring, pair, pair]


class Spread:
    def __init__(self, place, part, buf, send, recv):
        self.p, self.part, self.buf, self.send, self.recv = place, part, buf, send, recv

    def to(self, r):
        me = self.p.me
        return remote(self.part, self.buf.at[me], self.send.at[r], self.recv.at[me], lax.rem(me + r, self.p.n))

    def start(self):
        def one(r, _):
            self.to(r).start()
            return 0
        lax.fori_loop(1, self.p.n, one, 0)
        self.buf[pl.ds(self.p.me, 1)] = self.part[...][None]

    def total(self):
        def one(r, _):
            src = lax.rem(self.p.me + self.p.n - r, self.p.n)
            remote(self.part, self.buf.at[src], self.send.at[r], self.recv.at[src], src).wait_recv()
            return 0
        lax.fori_loop(1, self.p.n, one, 0)
        return lax.fori_loop(1, self.p.n, lambda j, acc: acc + self.buf[j], self.buf[0])

    def drain(self):
        def one(r, _):
            self.to(r).wait_send()
            return 0
        lax.fori_loop(1, self.p.n, one, 0)


class PairSpread:
    def __init__(self, place, part, other, half, buf, total, swap, pair_sems, send, recv):
        self.p, self.part, self.other, self.half, self.buf, self.sum, self.swap = place, part, other, half, buf, total, swap
        self.pair_sems, self.send, self.recv = pair_sems, send, recv
        self.rows = part.shape[0] // 2

    def pair(self, src, dst, i):
        return remote(src, dst, self.pair_sems.at[0, i], self.pair_sems.at[1, i], self.p.partner)

    def to(self, r):
        p = self.p
        return remote(self.half, self.buf.at[p.chip], self.send.at[r], self.recv.at[p.chip], lax.rem(p.me + 2 * r, p.n))

    def start(self):
        self.pair(self.part, self.other, 0).start()

    def across(self):
        self.pair(self.part, self.other, 0).wait_recv()
        both = self.part[...] + self.other[...]
        half = jnp.where(self.p.core == 0, both[:self.rows], both[self.rows:])
        self.half[...] = half
        self.buf[pl.ds(self.p.chip, 1)] = half[None]

        def one(r, _):
            self.to(r).start()
            return 0
        lax.fori_loop(1, self.p.chips, one, 0)

    def back(self):
        p = self.p

        def one(r, _):
            src = lax.rem(p.chip + p.chips - r, p.chips)
            remote(self.half, self.buf.at[src], self.send.at[r], self.recv.at[src], lax.rem(p.me + p.n - 2 * r, p.n)).wait_recv()
            return 0
        lax.fori_loop(1, p.chips, one, 0)
        self.sum[...] = lax.fori_loop(1, p.chips, lambda j, acc: acc + self.buf[j], self.buf[0])
        self.pair(self.sum, self.swap, 1).start()

    def total(self):
        self.pair(self.sum, self.swap, 1).wait_recv()
        mine, its = self.sum[...], self.swap[...]
        low = self.p.core == 0
        return jnp.concatenate([jnp.where(low, mine, its), jnp.where(low, its, mine)], axis=0)

    def drain(self):
        self.pair(self.part, self.other, 0).wait_send()
        self.pair(self.sum, self.swap, 1).wait_send()

        def one(r, _):
            self.to(r).wait_send()
            return 0
        lax.fori_loop(1, self.p.chips, one, 0)


def layer_kernel(n, loads, *refs):
    hbm, refs = refs[:loads], refs[loads:]
    gain2, bias2, gain1, bias1, dw1_hbm, dw2_hbm, db1_out, dwo_hbm, dx_out, dw_out, db_out, vec_out = refs[:12]
    x_mid, z, w1, w2, qT, kT, vT, wo, x_in, w_t = refs[12:12 + loads - 1]
    scratch = refs[12 + loads - 1:]
    load_sems, gy_buf, gh_buf = scratch[:3]
    rs_bufs, gathers, scatters, rest = scratch[3:9], scratch[9:25], scratch[25:33], scratch[33:]
    w1_t, w2_t, dw1_t, k_rows, lse, ctx_t, ctx_sum, dctx, dqkv_t, dk_acc, dv_acc, early, late_part = rest[:13]
    e_refs, (l_buf, l_send, l_recv), (dw1_out, dw2_out, dwo_out, db_acc, out_sems) = rest[13:21], rest[21:24], rest[24:]
    rows_here, width = x_mid.shape
    place = Place(n, rows_here)
    half, chips = place.half, place.chips
    seq = kT.shape[1]
    blk = seq // chips
    gy, gh, gm, g1 = (Gather(subs, place, buf, *gathers[4 * i:4 * i + 4]) for i, (subs, buf) in enumerate(((1, gy_buf), (1, gh_buf), (SUBS, gy_buf), (SUBS, gh_buf))))
    rs2, rs1 = (Scatter(subs, place, *rs_bufs, *scatters[4 * i:4 * i + 4]) for i, subs in enumerate((1, SUBS)))
    first_rows, last_rows = PairSpread(place, early, *e_refs), Spread(place, late_part, l_buf, l_send, l_recv)
    mine = pl.ds(pl.multiple_of(place.me * rows_here, rows_here), rows_here)
    way = [pl.ds(pl.multiple_of(place.me * rows_here + d * half, half), half) for d in (0, 1)]

    copies = [pltpu.make_async_copy(hbm[0], gy_buf.at[mine], load_sems.at[0])]
    copies += [pltpu.make_async_copy(hbm[i], refs[11 + i], load_sems.at[i]) for i in range(1, loads)]
    for c in copies:
        c.start()
    place.greet_all()
    copies[0].wait()
    gy.first()
    for c in copies[1:]:
        c.wait()
    gh_buf[mine, :] = layer_norm_fwd(x_mid[...], gain2[...], bias2[...])[2]
    w1_t[...] = w1[...].T
    w2_t[...] = w2[...].T
    for acc in (dw1_t, dw2_out, db1_out, dwo_out, dw_out, db_acc, dk_acc, dv_acc):
        acc[...] = jnp.zeros_like(acc)
    gh.first()

    def block(d, s, first):
        gy.arrive(d, s)
        dy = gy.load(d, s)
        pre = jnp.concatenate([z[place.span(d, s, True), :], z[place.span(d, s, False), :]], axis=0).astype(F32)
        act, slope = gelu_parts(pre)
        dz = (dot(dy, w2_t[...]) * slope).astype(BF16)
        rs2.put(d, s, dot(dz, w1_t[...]), first)
        if d == 1:
            rs2.give(0, s).start()
        dw2_out[...] += dot(act.astype(BF16).T, dy)
        db1_out[...] += jnp.sum(dz.astype(F32), axis=0, keepdims=True)
        return dz

    def late(d, s, dz):
        gh.arrive(d, s)
        dw1_t[...] += dot(dz.T, gh.load(d, s))

    def attend(s):
        attn_stats(s, blk, qT, kT, vT, k_rows, lse, ctx_t, ctx_sum)

    dz = [block(d, 0, True) for d in (0, 1)]
    rs2.give(1, 0).start()
    for d in (0, 1):
        late(d, 0, dz[d])
    attend(0)

    def mlp_step(s, _):
        gy.pass_on(s)
        dz = [block(d, s, False) for d in (0, 1)]

        @pl.when(s == chips - 1)
        def _():
            gy.drain()
        rs2.give(1, s).start()
        tail = rs2.pass_on(s)
        gh.pass_on(s)
        tail.start()
        for d in (0, 1):
            late(d, s, dz[d])
        attend(s)
        return 0
    lax.fori_loop(1, chips, mlp_step, 0)
    gh.drain()

    for d in (0, 1):
        rs2.own[d] = rs2.final(d, rs2.keep)
    vec = jnp.zeros((4, width), F32)
    for d in (0, 1):
        rows = slice(d * half, (d + 1) * half)
        x_hat, inv_std, _ = layer_norm_fwd(x_mid[rows, :], gain2[...], bias2[...])
        grad = rs2.own[d]
        dy = gy_buf[way[d], :].astype(F32)
        dmid = (dy + layer_norm_bwd(grad, x_hat, inv_std, gain2[...])).astype(BF16)
        gy_buf[way[d], :] = dmid
        vec += jnp.concatenate([jnp.sum(a, axis=0, keepdims=True) for a in (grad * x_hat, grad, dmid.astype(F32), dy)], axis=0)
        gm.first_way(d)
    early[...] = vec
    rs2.drain()
    first_rows.start()
    gh_buf[mine, :] = layer_norm_fwd(x_in[...], gain1[...], bias1[...])[2]

    def project(d, s):
        gm.arrive(d, s)
        rows = gm.load(d, s)
        both = dot_nt(wo[...], rows).astype(BF16)
        cols = [place.span(d, s, own) for own in (True, False)]
        dctx[:, cols[0]] = both[:, :half]
        dctx[:, cols[1]] = both[:, half:]
        dwo_out[...] += dot(jnp.concatenate([ctx_t[:, c] for c in cols], axis=1), rows)

    for d in (0, 1):
        project(d, 0)
    dw1_out[...] = dw1_t[...].T
    leave = [pltpu.make_async_copy(a, b, out_sems.at[i]) for i, (a, b) in enumerate(((dw2_out, dw2_hbm), (dw1_out, dw1_hbm), (dwo_out, dwo_hbm)))]
    leave[0].start()

    def mid_step(s, _):
        gm.pass_on(s)
        for d in (0, 1):
            project(d, s)
        return 0
    lax.fori_loop(1, chips - 1, mid_step, 0)
    gm.pass_on(chips - 1)
    g1.first()
    first_rows.across()
    leave[1].start()
    for d in (0, 1):
        project(d, chips - 1)

    stride = 3
    blocks = chips * (chips + 1) // 2
    events = g1.subs * (chips - 1)
    leave[2].start()
    left = list(range((blocks + stride - 1) // stride, events))

    def event(ev):
        g1.pass_one(1 + ev // g1.subs, ev % g1.subs if isinstance(ev, int) else lax.rem(ev, g1.subs))

    def service(e):
        ev = e // stride

        @pl.when((lax.rem(e, stride) == 0) & (ev < events))
        def _():
            event(ev)

    attn_grads(blk, qT, kT, vT, dctx, lse, ctx_sum, dqkv_t, k_rows, dk_acc, dv_acc, service)

    def cols_of(d, s):
        return jnp.concatenate([dqkv_t[:, place.span(d, s, own)] for own in (True, False)], axis=1)

    def back(s):
        for d in (0, 1):
            rows = cols_of(d, s).T
            rs1.put(d, s, dot(rows, w_t[...]))
            if d == 1:
                rs1.give(0, s).start()
            db_acc[...] += jnp.sum(rows.astype(F32), axis=0, keepdims=True)

    def weigh(d, s):
        g1.arrive(d, s)
        dw_out[...] += dot(cols_of(d, s), g1.load(d, s))

    for ev in left[:1]:
        event(ev)
    back(1)
    rs1.give(1, 1).start()
    for ev in left[1:]:
        event(ev)
    first_rows.back()

    def qkv_step(s, _):
        tail = rs1.pass_on(s)
        following = lax.rem(s + 1, chips)
        back(following)
        tail.start()
        rs1.give(1, following).start()
        for d in (0, 1):
            weigh(d, s - 1)
        return 0
    lax.fori_loop(1, chips, qkv_step, 0)

    vec = jnp.zeros((2, width), F32)
    for d in (0, 1):
        rows = slice(d * half, (d + 1) * half)
        x_hat, inv_std, _ = layer_norm_fwd(x_in[rows, :], gain1[...], bias1[...])
        grad = rs1.final(d, rs1.own)
        dx_out[rows, :] = (gy_buf[way[d], :].astype(F32) + layer_norm_bwd(grad, x_hat, inv_std, gain1[...])).astype(BF16)
        vec += jnp.concatenate([jnp.sum(grad * x_hat, axis=0, keepdims=True), jnp.sum(grad, axis=0, keepdims=True)], axis=0)
    late_part[...] = vec
    vec_out[2:6, :] = first_rows.total()
    last_rows.start()
    for d in (0, 1):
        weigh(d, chips - 1)
    vec_out[0:2, :] = last_rows.total()
    dim = qT.shape[0]
    for i in range(3):
        db_out[i] = db_acc[:, i * dim:(i + 1) * dim]
    for one in (gm, g1, rs1, first_rows, last_rows):
        one.drain()
    for c in leave:
        c.wait()


def layer_stage(n, dout, x_mid, z, w1, w2, q_t, k_t, v_t, wo, x_in, w_t, gain2, bias2, gain1, bias1):
    rows, width = dout.shape
    units = z.shape[1]
    dim, seq = q_t.shape
    hbm = (dout, x_mid, z, w1, w2, q_t, k_t, v_t, wo, x_in, w_t)
    vm = pl.BlockSpec(memory_space=pltpu.VMEM)
    full = pltpu.VMEM((n * rows, width), BF16)
    sem = pltpu.SemaphoreType.DMA((n,))
    acc = pltpu.VMEM((dim, seq), F32)
    scratch = [pltpu.VMEM(a.shape, a.dtype) for a in hbm[1:]] + [pltpu.SemaphoreType.DMA((len(hbm),)), full, full]
    scratch += scatter_bufs(n, rows, width) + gather_sems(n) * 4 + scatter_sems(n) * 2
    scratch += [pltpu.VMEM((units, width), BF16), pltpu.VMEM((width, units), BF16), pltpu.VMEM((units, width), F32),
                pltpu.VMEM((seq, dim), BF16), pltpu.VMEM((8, seq), F32), pltpu.VMEM((dim, seq), BF16), acc,
                pltpu.VMEM((dim, seq), BF16), pltpu.VMEM((3 * dim, seq), BF16), acc, acc,
                pltpu.VMEM((4, width), F32), pltpu.VMEM((2, width), F32),
                pltpu.VMEM((4, width), F32), pltpu.VMEM((2, width), F32), pltpu.VMEM((n // 2, 2, width), F32), pltpu.VMEM((2, width), F32),
                pltpu.VMEM((2, width), F32), pltpu.SemaphoreType.DMA((2, 2)), pltpu.SemaphoreType.DMA((n // 2,)), pltpu.SemaphoreType.DMA((n // 2,)),
                pltpu.VMEM((n, 2, width), F32), sem, sem,
                pltpu.VMEM((width, units), F32), pltpu.VMEM((units, width), F32), pltpu.VMEM((dim, width), F32), pltpu.VMEM((1, 3 * dim), F32),
                pltpu.SemaphoreType.DMA((3,))]
    outs = [((width, units), F32), ((units, width), F32), ((1, units), F32), ((dim, width), F32), ((rows, width), BF16),
            (w_t.shape, F32), ((3, 1, dim), F32), ((6, width), F32)]
    return pl.pallas_call(
        functools.partial(layer_kernel, n, len(hbm)),
        in_specs=[pl.BlockSpec(memory_space=pl.ANY)] * len(hbm) + [vm] * 4,
        out_specs=[pl.BlockSpec(memory_space=pl.ANY) if i in (0, 1, 3) else vm for i in range(len(outs))],
        out_shape=[jax.ShapeDtypeStruct(*o) for o in outs],
        scratch_shapes=scratch,
        compiler_params=pltpu.CompilerParams(collective_id=1, has_side_effects=True, vmem_limit_bytes=67043328),
        name="layer_stage",
    )(*hbm, gain2, bias2, gain1, bias1)


def deliver_kernel(pieces, *refs):
    count = (len(refs) - 2) // 3
    src, dst, buf, (in_sem, out_sem) = refs[:count], refs[count:2 * count], refs[2 * count:3 * count], refs[3 * count:]
    into, out = [], []
    for i in range(count):
        size = src[i].shape[0] // pieces[i]
        for j in range(pieces[i]):
            rows = slice(j * size, (j + 1) * size)
            into.append(pltpu.make_async_copy(src[i].at[rows], buf[i].at[rows], in_sem.at[len(into)]))
            out.append(pltpu.make_async_copy(buf[i].at[rows], dst[i].at[rows], out_sem.at[len(out)]))
    for c in into:
        c.start()
    for a, b in zip(into, out):
        a.wait()
        b.start()
    for b in out:
        b.wait()


def deliver(arrays):
    pieces = [2 if a.ndim == 2 and a.shape[0] % 32 == 0 else 1 for a in arrays]
    sems = pltpu.SemaphoreType.DMA((sum(pieces),))
    return pl.pallas_call(
        functools.partial(deliver_kernel, pieces),
        in_specs=[pl.BlockSpec(memory_space=pl.ANY)] * len(arrays),
        out_specs=[pl.BlockSpec(memory_space=pl.ANY)] * len(arrays),
        out_shape=[jax.ShapeDtypeStruct(a.shape, a.dtype) for a in arrays],
        scratch_shapes=[pltpu.VMEM(a.shape, a.dtype) for a in arrays] + [sems, sems],
        compiler_params=pltpu.CompilerParams(vmem_limit_bytes=67043328),
        name="deliver",
    )(*arrays)


def solution(mesh):
    def local_backward(x_in, x_mid, d_out, q_saved, k_saved, v_saved, z_saved, ln1_gain, ln1_bias, ln2_gain, ln2_bias, w_qkv, w_proj, w_fc1, w_fc2):
        n = mesh.shape['tp']
        dim = q_saved.shape[-1]
        row = lambda a: a[None, :]
        q_t, k_t, v_t = (jnp.transpose(a[0, :, 0, :]) for a in (q_saved, k_saved, v_saved))
        w_qkv_t = jnp.transpose(w_qkv[:, :, 0, :], (0, 2, 1)).reshape(3 * dim, -1)
        dw1, dw2, db1, dwo, dx, dw_t, db, vecs = layer_stage(
            n, d_out[0], x_mid[0], z_saved[0], w_fc1, w_fc2, q_t, k_t, v_t, w_proj[0], x_in[0], w_qkv_t,
            row(ln2_gain), row(ln2_bias), row(ln1_gain), row(ln1_bias))
        dw1, dw2, dwo, dw_t, dx, db1, db, vecs = deliver((dw1, dw2, dwo, dw_t, dx, db1, db, vecs))
        grad_wqkv = jnp.transpose(dw_t.reshape(3, dim, -1), (0, 2, 1))[:, :, None, :]
        return dx[None], grad_wqkv, db, dwo[None], dw1, db1[0], dw2, vecs

    tok_spec = P('dp', 'tp', None)
    head_spec = P('dp', None, 'tp', None)
    in_specs = (tok_spec, tok_spec, tok_spec, head_spec, head_spec, head_spec, P('dp', None, 'tp'),
                P(None), P(None), P(None), P(None),
                P(None, None, 'tp', None), P('tp', None, None), P(None, 'tp'), P('tp', None))
    out_specs = (tok_spec, P('dp', None, 'tp', None), P('dp', 'tp', None), P(('dp', 'tp'), None, None),
                 P('dp', 'tp'), P(('dp', 'tp')), P(('dp', 'tp'), None), P('dp', None))
    return jax.shard_map(local_backward, mesh=mesh, in_specs=in_specs, out_specs=out_specs, check_vma=False)
```

```python
import functools
import jax, jax.numpy as jnp
from jax import lax
from jax.experimental import pallas as pl
from jax.experimental.pallas import tpu as pltpu
from jax.sharding import PartitionSpec as P

F32, BF16 = jnp.float32, jnp.bfloat16
LOG2E = 1.4426950408889634
LN_EPS = 1e-5
GELU_COEF = 0.044715
GELU_SCALE = 0.7978845608028654


def dot(a, b):
    return lax.dot_general(a, b, (((1,), (0,)), ((), ())), preferred_element_type=F32)


def layer_norm_fwd(token_rows, norm_gain, norm_bias):
    rows_f32 = token_rows.astype(jnp.float32)
    centered = rows_f32 - jnp.mean(rows_f32, axis=-1, keepdims=True)
    inv_std = lax.rsqrt(jnp.mean(centered * centered, axis=-1, keepdims=True) + LN_EPS)
    x_hat = centered * inv_std
    return x_hat, inv_std, (x_hat * norm_gain + norm_bias).astype(jnp.bfloat16)


def layer_norm_bwd(grad_norm, x_hat, inv_std, norm_gain):
    grad_hat = grad_norm * norm_gain
    centered_grad = grad_hat - jnp.mean(grad_hat, axis=-1, keepdims=True)
    return inv_std * (centered_grad - x_hat * jnp.mean(grad_hat * x_hat, axis=-1, keepdims=True))


def gelu_parts(pre_act):
    tanh_val = jnp.tanh(GELU_SCALE * (pre_act + GELU_COEF * pre_act * pre_act * pre_act))
    act_value = 0.5 * pre_act * (1.0 + tanh_val)
    act_slope = 0.5 * (1.0 + tanh_val) + 0.5 * pre_act * (1.0 - tanh_val * tanh_val) * GELU_SCALE * (1.0 + 3.0 * GELU_COEF * pre_act * pre_act)
    return act_value, act_slope


def attn_stats(step, blk, qT, kT, vT, k_rows, lse_out, ctx_out, sum_out):
    dim, seq = kT.shape
    c = (dim ** -0.5) * LOG2E
    here = pl.ds(pl.multiple_of(step * blk, blk), blk)
    q = qT[:, here]
    k_rows[here, :] = kT[:, here].T

    def scores(i, masked):
        rows = pl.ds(pl.multiple_of(i * blk, blk), blk)
        s = dot(k_rows[rows, :], q) * c
        if masked:
            r = lax.broadcasted_iota(jnp.int32, (blk, blk), 0)
            col = lax.broadcasted_iota(jnp.int32, (blk, blk), 1)
            s = jnp.where(r <= col, s, -1e30)
        return s

    def stats(i, carry, masked):
        m, l = carry
        s = scores(i, masked)
        new = jnp.maximum(m, jnp.max(s, axis=0, keepdims=True))
        l = l * jnp.exp2(m - new) + jnp.sum(jnp.exp2(s - new), axis=0, keepdims=True)
        return new, l

    init = (jnp.full((1, blk), -1e30, F32), jnp.zeros((1, blk), F32))
    carry = lax.fori_loop(0, step, functools.partial(stats, masked=False), init)
    m, l = stats(step, carry, True)
    lse = m + jnp.log2(l)

    def apply(i, carry, masked):
        low_sum, res_sum = carry
        p = jnp.exp2(scores(i, masked) - lse)
        low = p.astype(BF16)
        res = (p - low.astype(F32)).astype(BF16)
        v = vT[:, pl.ds(pl.multiple_of(i * blk, blk), blk)]
        return low_sum + dot(v, low), res_sum + dot(v, res)

    zero = jnp.zeros((dim, blk), F32)
    carry = lax.fori_loop(0, step, functools.partial(apply, masked=False), (zero, zero))
    low_sum, res_sum = apply(step, carry, True)
    ctx_out[:, here] = low_sum.astype(BF16)
    sum_out[:, here] = low_sum + res_sum
    lse_out[:, here] = jnp.broadcast_to(lse, (8, blk))


def attn_grads(blk, qT, kT, vT, dctxT, lse, ctxsum, out, k_rows, dk_acc, dv_acc, service):
    dim, seq = kT.shape
    scale = dim ** -0.5
    c = scale * LOG2E

    def queries(step, _):
        here = pl.ds(pl.multiple_of(step * blk, blk), blk)
        qt = qT[:, here]
        dct = dctxT[:, here]
        q = qt.T
        dc = dct.T
        delta_row = jnp.sum(dct.astype(F32) * ctxsum[:, here], axis=0, keepdims=True)
        lse_col = jnp.broadcast_to(lse[0:1, here], (128, blk)).T[:, :1]
        delta_col = jnp.broadcast_to(delta_row, (128, blk)).T[:, :1]
        base = step * (step + 1) // 2

        def block(i, dq, masked):
            service(base + i)
            cols = pl.ds(pl.multiple_of(i * blk, blk), blk)
            s = dot(q, kT[:, cols]) * c
            dp = dot(dc, vT[:, cols])
            p = jnp.exp2(s - lse_col)
            if masked:
                r = lax.broadcasted_iota(jnp.int32, (blk, blk), 0)
                col = lax.broadcasted_iota(jnp.int32, (blk, blk), 1)
                p = jnp.where(r >= col, p, 0.0)
            ds = (p * (dp - delta_col)).astype(BF16)
            dv_acc[:, cols] += dot(dct, p.astype(BF16))
            dk_acc[:, cols] += dot(qt, ds)
            return dq + dot(ds, k_rows[cols, :])

        dq = lax.fori_loop(0, step, functools.partial(block, masked=False), jnp.zeros((blk, dim), F32))
        dq = block(step, dq, True)
        out[0:dim, here] = (dq * scale).T.astype(BF16)
        return 0
    lax.fori_loop(0, seq // blk, queries, 0)

    def put(i, _):
        cols = pl.ds(pl.multiple_of(i * blk, blk), blk)
        out[dim:2 * dim, cols] = (dk_acc[:, cols] * scale).astype(BF16)
        out[2 * dim:3 * dim, cols] = dv_acc[:, cols].astype(BF16)
        return 0
    lax.fori_loop(0, seq // blk, put, 0)


MESH = pl.DeviceIdType.MESH
SUBS = 4


def dot_nt(a, b):
    return lax.dot_general(a, b, (((1,), (1,)), ((), ())), preferred_element_type=F32)


def remote(src, dst, send_sem, recv_sem, dev):
    return pltpu.make_async_remote_copy(src_ref=src, dst_ref=dst, send_sem=send_sem, recv_sem=recv_sem,
                                        device_id={'tp': dev}, device_id_type=MESH)


class Place:
    def __init__(self, n, rows):
        me = lax.axis_index('tp')
        self.me, self.n, self.chips, self.half, self.rows = me, n, n // 2, rows // 2, rows
        self.core, self.chip = lax.rem(me, 2), me // 2
        self.partner = me + 1 - 2 * self.core
        self.next = (lax.rem(me + 2, n), lax.rem(me + n - 2, n))

    def origin(self, d, s):
        return lax.rem(self.chip + (self.chips - s if d == 0 else s), self.chips)

    def span(self, d, s, own):
        core = self.core if own else 1 - self.core
        start = (2 * self.origin(d, s) + core) * self.rows + d * self.half
        return pl.ds(pl.multiple_of(start, self.half), self.half)

    def part(self, d, s, own, sub, subs):
        core, size = self.core if own else 1 - self.core, self.half // subs
        start = (2 * self.origin(d, s) + core) * self.rows + d * self.half + sub * size
        return pl.ds(pl.multiple_of(start, size), size)

    def greet(self):
        barrier = pltpu.get_barrier_semaphore()
        for dev in (self.next[0], self.next[1], self.partner):
            pl.semaphore_signal(barrier, inc=1, device_id={'tp': dev}, device_id_type=MESH)
        pl.semaphore_wait(barrier, 3)

    def greet_all(self):
        barrier = pltpu.get_barrier_semaphore()

        def hello(r, _):
            pl.semaphore_signal(barrier, inc=1, device_id={'tp': lax.rem(self.me + r, self.n)}, device_id_type=MESH)
            return 0
        lax.fori_loop(1, self.n, hello, 0)
        pl.semaphore_wait(barrier, self.n - 1)


class Gather:
    def __init__(self, subs, place, buf, send, recv, psend, precv):
        self.subs, self.p, self.buf, self.send, self.recv, self.psend, self.precv = subs, place, buf, send, recv, psend, precv

    def hop(self, d, s, sub):
        at = self.buf.at[self.p.part(d, s, True, sub, self.subs)]
        return remote(at, at, self.send.at[d, s, sub], self.recv.at[d, s, sub], self.p.next[d])

    def give(self, d, s, sub):
        at = self.buf.at[self.p.part(d, s, True, sub, self.subs)]
        return remote(at, at, self.psend.at[d, s, sub], self.precv.at[d, s, sub], self.p.partner)

    def first_way(self, d):
        for sub in range(self.subs):
            self.hop(d, 0, sub).start()
            self.give(d, 0, sub).start()

    def first(self):
        for sub in range(self.subs):
            for d in (0, 1):
                self.hop(d, 0, sub).start()
        for sub in range(self.subs):
            for d in (0, 1):
                self.give(d, 0, sub).start()

    def pass_one(self, s, sub):
        for d in (0, 1):
            at = self.buf.at[self.p.part(d, s, True, sub, self.subs)]
            remote(at, at, self.send.at[d, s - 1, sub], self.recv.at[d, s - 1, sub], self.p.next[d]).wait_recv()

            @pl.when(s < self.p.chips - 1)
            def _():
                self.hop(d, s, sub).start()
            self.give(d, s, sub).start()

    def pass_on(self, s):
        for sub in range(self.subs):
            self.pass_one(s, sub)

    def arrive(self, d, s):
        for sub in range(self.subs):
            at = self.buf.at[self.p.part(d, s, False, sub, self.subs)]
            remote(at, at, self.psend.at[d, s, sub], self.precv.at[d, s, sub], self.p.partner).wait_recv()

    def load(self, d, s):
        return jnp.concatenate([self.buf[self.p.span(d, s, True), :], self.buf[self.p.span(d, s, False), :]], axis=0)

    def drain(self):
        def one(s, _):
            for d in (0, 1):
                for sub in range(self.subs):
                    self.give(d, s, sub).wait_send()

                    @pl.when(s < self.p.chips - 1)
                    def _():
                        self.hop(d, s, sub).wait_send()
            return 0
        lax.fori_loop(0, self.p.chips, one, 0)


class Scatter:
    def __init__(self, subs, place, own, keep, out, inc, pout, pinc, send, recv, psend, precv):
        self.subs, self.size = subs, place.half // subs
        self.p, self.own, self.keep, self.out, self.inc, self.send, self.recv = place, own, keep, out, inc, send, recv
        self.pout, self.pinc, self.psend, self.precv = pout, pinc, psend, precv

    def give(self, d, s):
        return remote(self.pout.at[d, s], self.pinc.at[d, s], self.psend.at[d, s], self.precv.at[d, s], self.p.partner)

    def hop(self, d, r, sub):
        rows = slice(sub * self.size, (sub + 1) * self.size)
        return remote(self.out.at[d, r, rows], self.inc.at[d, r, rows], self.send.at[d, r, sub], self.recv.at[d, r, sub], self.p.next[d])

    def put(self, d, s, part, first=False):
        half = self.p.half
        (self.keep if first else self.own)[d] = part[:half]
        self.pout[d, s] = part[half:].astype(BF16)

    def join(self, d, s):
        self.give(d, s).wait_recv()
        self.own[d] += self.pinc[d, s].astype(F32)

    def forward(self, d, s, sub):
        rows = slice(sub * self.size, (sub + 1) * self.size)

        @pl.when(s >= 2)
        def _():
            self.hop(d, s - 2, sub).wait_recv()
            self.out[d, s - 1, rows] = (self.own[d, rows] + self.inc[d, s - 2, rows].astype(F32)).astype(BF16)

        @pl.when(s < 2)
        def _():
            self.out[d, s - 1, rows] = self.own[d, rows].astype(BF16)

    def pass_on(self, s):
        for d in (0, 1):
            self.join(d, s)
        before = None
        for sub in range(self.subs):
            for d in (0, 1):
                self.forward(d, s, sub)
                if before is not None:
                    self.hop(*before).start()
                before = (d, s - 1, sub)
        return self.hop(*before)

    def final(self, d, store):
        last = self.p.chips - 2
        self.give(d, 0).wait_recv()
        for sub in range(self.subs):
            self.hop(d, last, sub).wait_recv()
        return store[d] + self.pinc[d, 0].astype(F32) + self.inc[d, last].astype(F32)

    def drain(self):
        def one(s, _):
            for d in (0, 1):
                self.give(d, s).wait_send()
                for sub in range(self.subs):
                    @pl.when(s < self.p.chips - 1)
                    def _():
                        self.hop(d, s, sub).wait_send()
            return 0
        lax.fori_loop(0, self.p.chips, one, 0)


def gather_sems(n):
    return [pltpu.SemaphoreType.DMA((2, n // 2, SUBS))] * 4


def scatter_sems(n):
    sem = pltpu.SemaphoreType.DMA((2, n // 2))
    fine = pltpu.SemaphoreType.DMA((2, n // 2, SUBS))
    return [fine, fine, sem, sem]


def scatter_bufs(n, rows, width):
    chips, half = n // 2, rows // 2
    wide = pltpu.VMEM((2, half, width), F32)
    ring = pltpu.VMEM((2, chips - 1, half, width), BF16)
    pair = pltpu.VMEM((2, chips, half, width), BF16)
    return [wide, wide, ring, ring, pair, pair]


class Spread:
    def __init__(self, place, part, buf, send, recv):
        self.p, self.part, self.buf, self.send, self.recv = place, part, buf, send, recv

    def to(self, r):
        me = self.p.me
        return remote(self.part, self.buf.at[me], self.send.at[r], self.recv.at[me], lax.rem(me + r, self.p.n))

    def start(self):
        def one(r, _):
            self.to(r).start()
            return 0
        lax.fori_loop(1, self.p.n, one, 0)
        self.buf[pl.ds(self.p.me, 1)] = self.part[...][None]

    def total(self):
        def one(r, _):
            src = lax.rem(self.p.me + self.p.n - r, self.p.n)
            remote(self.part, self.buf.at[src], self.send.at[r], self.recv.at[src], src).wait_recv()
            return 0
        lax.fori_loop(1, self.p.n, one, 0)
        return lax.fori_loop(1, self.p.n, lambda j, acc: acc + self.buf[j], self.buf[0])

    def drain(self):
        def one(r, _):
            self.to(r).wait_send()
            return 0
        lax.fori_loop(1, self.p.n, one, 0)


class PairSpread:
    def __init__(self, place, part, other, half, buf, total, swap, pair_sems, send, recv):
        self.p, self.part, self.other, self.half, self.buf, self.sum, self.swap = place, part, other, half, buf, total, swap
        self.pair_sems, self.send, self.recv = pair_sems, send, recv
        self.rows = part.shape[0] // 2

    def pair(self, src, dst, i):
        return remote(src, dst, self.pair_sems.at[0, i], self.pair_sems.at[1, i], self.p.partner)

    def to(self, r):
        p = self.p
        return remote(self.half, self.buf.at[p.chip], self.send.at[r], self.recv.at[p.chip], lax.rem(p.me + 2 * r, p.n))

    def start(self):
        self.pair(self.part, self.other, 0).start()

    def across(self):
        self.pair(self.part, self.other, 0).wait_recv()
        both = self.part[...] + self.other[...]
        half = jnp.where(self.p.core == 0, both[:self.rows], both[self.rows:])
        self.half[...] = half
        self.buf[pl.ds(self.p.chip, 1)] = half[None]

        def one(r, _):
            self.to(r).start()
            return 0
        lax.fori_loop(1, self.p.chips, one, 0)

    def back(self):
        p = self.p

        def one(r, _):
            src = lax.rem(p.chip + p.chips - r, p.chips)
            remote(self.half, self.buf.at[src], self.send.at[r], self.recv.at[src], lax.rem(p.me + p.n - 2 * r, p.n)).wait_recv()
            return 0
        lax.fori_loop(1, p.chips, one, 0)
        self.sum[...] = lax.fori_loop(1, p.chips, lambda j, acc: acc + self.buf[j], self.buf[0])
        self.pair(self.sum, self.swap, 1).start()

    def total(self):
        self.pair(self.sum, self.swap, 1).wait_recv()
        mine, its = self.sum[...], self.swap[...]
        low = self.p.core == 0
        return jnp.concatenate([jnp.where(low, mine, its), jnp.where(low, its, mine)], axis=0)

    def drain(self):
        self.pair(self.part, self.other, 0).wait_send()
        self.pair(self.sum, self.swap, 1).wait_send()

        def one(r, _):
            self.to(r).wait_send()
            return 0
        lax.fori_loop(1, self.p.chips, one, 0)


def layer_kernel(n, loads, *refs):
    hbm, refs = refs[:loads], refs[loads:]
    gain2, bias2, gain1, bias1, dw1_hbm, dw2_hbm, db1_out, dwo_hbm, dx_out, dw_out, db_out, vec_out = refs[:12]
    x_mid, z, w1, w2, qT, kT, vT, wo, x_in, w_t = refs[12:12 + loads - 1]
    scratch = refs[12 + loads - 1:]
    load_sems, gy_buf, gh_buf = scratch[:3]
    rs_bufs, gathers, scatters, rest = scratch[3:9], scratch[9:25], scratch[25:33], scratch[33:]
    w1_t, w2_t, dw1_t, k_rows, lse, ctx_t, ctx_sum, dctx, dqkv_t, dk_acc, dv_acc, early, late_part = rest[:13]
    e_refs, (l_buf, l_send, l_recv), (dw1_out, dw2_out, dwo_out, db_acc, out_sems) = rest[13:21], rest[21:24], rest[24:]
    rows_here, width = x_mid.shape
    place = Place(n, rows_here)
    half, chips = place.half, place.chips
    seq = kT.shape[1]
    blk = seq // chips
    gy, gh, gm, g1 = (Gather(subs, place, buf, *gathers[4 * i:4 * i + 4]) for i, (subs, buf) in enumerate(((1, gy_buf), (1, gh_buf), (2, gy_buf), (2, gh_buf))))
    rs2, rs1 = (Scatter(subs, place, *rs_bufs, *scatters[4 * i:4 * i + 4]) for i, subs in enumerate((1, SUBS)))
    first_rows, last_rows = PairSpread(place, early, *e_refs), Spread(place, late_part, l_buf, l_send, l_recv)
    mine = pl.ds(pl.multiple_of(place.me * rows_here, rows_here), rows_here)
    way = [pl.ds(pl.multiple_of(place.me * rows_here + d * half, half), half) for d in (0, 1)]

    copies = [pltpu.make_async_copy(hbm[0], gy_buf.at[mine], load_sems.at[0])]
    copies += [pltpu.make_async_copy(hbm[i], refs[11 + i], load_sems.at[i]) for i in range(1, loads)]
    for c in copies:
        c.start()
    place.greet_all()
    copies[0].wait()
    gy.first()
    for c in copies[1:]:
        c.wait()
    gh_buf[mine, :] = layer_norm_fwd(x_mid[...], gain2[...], bias2[...])[2]
    w1_t[...] = w1[...].T
    w2_t[...] = w2[...].T
    for acc in (dw1_t, dw2_out, db1_out, dwo_out, dw_out, db_acc, dk_acc, dv_acc):
        acc[...] = jnp.zeros_like(acc)
    gh.first()

    def block(d, s, first):
        gy.arrive(d, s)
        dy = gy.load(d, s)
        pre = jnp.concatenate([z[place.span(d, s, True), :], z[place.span(d, s, False), :]], axis=0).astype(F32)
        act, slope = gelu_parts(pre)
        dz = (dot(dy, w2_t[...]) * slope).astype(BF16)
        rs2.put(d, s, dot(dz, w1_t[...]), first)
        if d == 1:
            rs2.give(0, s).start()
        dw2_out[...] += dot(act.astype(BF16).T, dy)
        db1_out[...] += jnp.sum(dz.astype(F32), axis=0, keepdims=True)
        return dz

    def late(d, s, dz):
        gh.arrive(d, s)
        dw1_t[...] += dot(dz.T, gh.load(d, s))

    def attend(s):
        attn_stats(s, blk, qT, kT, vT, k_rows, lse, ctx_t, ctx_sum)

    dz = [block(d, 0, True) for d in (0, 1)]
    rs2.give(1, 0).start()
    for d in (0, 1):
        late(d, 0, dz[d])
    attend(0)

    def mlp_step(s, _):
        gy.pass_on(s)
        dz = [block(d, s, False) for d in (0, 1)]

        @pl.when(s == chips - 1)
        def _():
            gy.drain()
        rs2.give(1, s).start()
        tail = rs2.pass_on(s)
        gh.pass_on(s)
        tail.start()
        for d in (0, 1):
            late(d, s, dz[d])
        attend(s)
        return 0
    lax.fori_loop(1, chips, mlp_step, 0)
    gh.drain()

    for d in (0, 1):
        rs2.own[d] = rs2.final(d, rs2.keep)
    vec = jnp.zeros((4, width), F32)
    for d in (0, 1):
        rows = slice(d * half, (d + 1) * half)
        x_hat, inv_std, _ = layer_norm_fwd(x_mid[rows, :], gain2[...], bias2[...])
        grad = rs2.own[d]
        dy = gy_buf[way[d], :].astype(F32)
        dmid = (dy + layer_norm_bwd(grad, x_hat, inv_std, gain2[...])).astype(BF16)
        gy_buf[way[d], :] = dmid
        vec += jnp.concatenate([jnp.sum(a, axis=0, keepdims=True) for a in (grad * x_hat, grad, dmid.astype(F32), dy)], axis=0)
        gm.first_way(d)
    early[...] = vec
    rs2.drain()
    first_rows.start()
    gh_buf[mine, :] = layer_norm_fwd(x_in[...], gain1[...], bias1[...])[2]

    def project(d, s):
        gm.arrive(d, s)
        rows = gm.load(d, s)
        both = dot_nt(wo[...], rows).astype(BF16)
        cols = [place.span(d, s, own) for own in (True, False)]
        dctx[:, cols[0]] = both[:, :half]
        dctx[:, cols[1]] = both[:, half:]
        dwo_out[...] += dot(jnp.concatenate([ctx_t[:, c] for c in cols], axis=1), rows)

    for d in (0, 1):
        project(d, 0)
    dw1_out[...] = dw1_t[...].T
    leave = [pltpu.make_async_copy(a, b, out_sems.at[i]) for i, (a, b) in enumerate(((dw2_out, dw2_hbm), (dw1_out, dw1_hbm), (dwo_out, dwo_hbm)))]
    leave[0].start()

    def mid_step(s, _):
        gm.pass_on(s)
        for d in (0, 1):
            project(d, s)
        return 0
    lax.fori_loop(1, chips - 1, mid_step, 0)
    gm.pass_on(chips - 1)
    g1.first()
    first_rows.across()
    leave[1].start()
    for d in (0, 1):
        project(d, chips - 1)

    stride = 3
    blocks = chips * (chips + 1) // 2
    events = g1.subs * (chips - 1)
    leave[2].start()
    left = list(range((blocks + stride - 1) // stride, events))

    def event(ev):
        g1.pass_one(1 + ev // g1.subs, ev % g1.subs if isinstance(ev, int) else lax.rem(ev, g1.subs))

    def service(e):
        ev = e // stride

        @pl.when((lax.rem(e, stride) == 0) & (ev < events))
        def _():
            event(ev)

    attn_grads(blk, qT, kT, vT, dctx, lse, ctx_sum, dqkv_t, k_rows, dk_acc, dv_acc, service)

    def cols_of(d, s):
        return jnp.concatenate([dqkv_t[:, place.span(d, s, own)] for own in (True, False)], axis=1)

    def back(s):
        for d in (0, 1):
            rows = cols_of(d, s).T
            rs1.put(d, s, dot(rows, w_t[...]))
            if d == 1:
                rs1.give(0, s).start()
            db_acc[...] += jnp.sum(rows.astype(F32), axis=0, keepdims=True)

    def weigh(d, s):
        g1.arrive(d, s)
        dw_out[...] += dot(cols_of(d, s), g1.load(d, s))

    for ev in left[:1]:
        event(ev)
    back(1)
    rs1.give(1, 1).start()
    for ev in left[1:]:
        event(ev)
    first_rows.back()

    def qkv_step(s, _):
        tail = rs1.pass_on(s)
        following = lax.rem(s + 1, chips)
        back(following)
        tail.start()
        rs1.give(1, following).start()
        for d in (0, 1):
            weigh(d, s - 1)
        return 0
    lax.fori_loop(1, chips, qkv_step, 0)

    inv_stds = []
    for d in (0, 1):
        x_hat, inv_std, _ = layer_norm_fwd(x_in[d * half:(d + 1) * half, :], gain1[...], bias1[...])
        rs1.keep[d] = x_hat
        inv_stds.append(inv_std)
    vec = jnp.zeros((2, width), F32)
    for d in (0, 1):
        rows = slice(d * half, (d + 1) * half)
        grad = rs1.final(d, rs1.own)
        x_hat, inv_std = rs1.keep[d], inv_stds[d]
        dx_out[rows, :] = (gy_buf[way[d], :].astype(F32) + layer_norm_bwd(grad, x_hat, inv_std, gain1[...])).astype(BF16)
        vec += jnp.concatenate([jnp.sum(grad * x_hat, axis=0, keepdims=True), jnp.sum(grad, axis=0, keepdims=True)], axis=0)
    late_part[...] = vec
    vec_out[2:6, :] = first_rows.total()
    last_rows.start()
    for d in (0, 1):
        weigh(d, chips - 1)
    vec_out[0:2, :] = last_rows.total()
    dim = qT.shape[0]
    for i in range(3):
        db_out[i] = db_acc[:, i * dim:(i + 1) * dim]
    for one in (gm, g1, rs1, first_rows, last_rows):
        one.drain()
    for c in leave:
        c.wait()


def layer_stage(n, dout, x_mid, z, w1, w2, q_t, k_t, v_t, wo, x_in, w_t, gain2, bias2, gain1, bias1):
    rows, width = dout.shape
    units = z.shape[1]
    dim, seq = q_t.shape
    hbm = (dout, x_mid, z, w1, w2, q_t, k_t, v_t, wo, x_in, w_t)
    vm = pl.BlockSpec(memory_space=pltpu.VMEM)
    full = pltpu.VMEM((n * rows, width), BF16)
    sem = pltpu.SemaphoreType.DMA((n,))
    acc = pltpu.VMEM((dim, seq), F32)
    scratch = [pltpu.VMEM(a.shape, a.dtype) for a in hbm[1:]] + [pltpu.SemaphoreType.DMA((len(hbm),)), full, full]
    scratch += scatter_bufs(n, rows, width) + gather_sems(n) * 4 + scatter_sems(n) * 2
    scratch += [pltpu.VMEM((units, width), BF16), pltpu.VMEM((width, units), BF16), pltpu.VMEM((units, width), F32),
                pltpu.VMEM((seq, dim), BF16), pltpu.VMEM((8, seq), F32), pltpu.VMEM((dim, seq), BF16), acc,
                pltpu.VMEM((dim, seq), BF16), pltpu.VMEM((3 * dim, seq), BF16), acc, acc,
                pltpu.VMEM((4, width), F32), pltpu.VMEM((2, width), F32),
                pltpu.VMEM((4, width), F32), pltpu.VMEM((2, width), F32), pltpu.VMEM((n // 2, 2, width), F32), pltpu.VMEM((2, width), F32),
                pltpu.VMEM((2, width), F32), pltpu.SemaphoreType.DMA((2, 2)), pltpu.SemaphoreType.DMA((n // 2,)), pltpu.SemaphoreType.DMA((n // 2,)),
                pltpu.VMEM((n, 2, width), F32), sem, sem,
                pltpu.VMEM((width, units), F32), pltpu.VMEM((units, width), F32), pltpu.VMEM((dim, width), F32), pltpu.VMEM((1, 3 * dim), F32),
                pltpu.SemaphoreType.DMA((3,))]
    outs = [((width, units), F32), ((units, width), F32), ((1, units), F32), ((dim, width), F32), ((rows, width), BF16),
            (w_t.shape, F32), ((3, 1, dim), F32), ((6, width), F32)]
    return pl.pallas_call(
        functools.partial(layer_kernel, n, len(hbm)),
        in_specs=[pl.BlockSpec(memory_space=pl.ANY)] * len(hbm) + [vm] * 4,
        out_specs=[pl.BlockSpec(memory_space=pl.ANY) if i in (0, 1, 3) else vm for i in range(len(outs))],
        out_shape=[jax.ShapeDtypeStruct(*o) for o in outs],
        scratch_shapes=scratch,
        compiler_params=pltpu.CompilerParams(collective_id=1, has_side_effects=True, vmem_limit_bytes=67043328),
        name="layer_stage",
    )(*hbm, gain2, bias2, gain1, bias1)


def deliver_kernel(pieces, *refs):
    count = (len(refs) - 2) // 3
    src, dst, buf, (in_sem, out_sem) = refs[:count], refs[count:2 * count], refs[2 * count:3 * count], refs[3 * count:]
    into, out = [], []
    for i in range(count):
        size = src[i].shape[0] // pieces[i]
        for j in range(pieces[i]):
            rows = slice(j * size, (j + 1) * size)
            into.append(pltpu.make_async_copy(src[i].at[rows], buf[i].at[rows], in_sem.at[len(into)]))
            out.append(pltpu.make_async_copy(buf[i].at[rows], dst[i].at[rows], out_sem.at[len(out)]))
    for c in into:
        c.start()
    for a, b in zip(into, out):
        a.wait()
        b.start()
    for b in out:
        b.wait()


def deliver(arrays):
    pieces = [2 if a.ndim == 2 and a.shape[0] % 32 == 0 else 1 for a in arrays]
    sems = pltpu.SemaphoreType.DMA((sum(pieces),))
    return pl.pallas_call(
        functools.partial(deliver_kernel, pieces),
        in_specs=[pl.BlockSpec(memory_space=pl.ANY)] * len(arrays),
        out_specs=[pl.BlockSpec(memory_space=pl.ANY)] * len(arrays),
        out_shape=[jax.ShapeDtypeStruct(a.shape, a.dtype) for a in arrays],
        scratch_shapes=[pltpu.VMEM(a.shape, a.dtype) for a in arrays] + [sems, sems],
        compiler_params=pltpu.CompilerParams(vmem_limit_bytes=67043328),
        name="deliver",
    )(*arrays)


def solution(mesh):
    def local_backward(x_in, x_mid, d_out, q_saved, k_saved, v_saved, z_saved, ln1_gain, ln1_bias, ln2_gain, ln2_bias, w_qkv, w_proj, w_fc1, w_fc2):
        n = mesh.shape['tp']
        dim = q_saved.shape[-1]
        row = lambda a: a[None, :]
        q_t, k_t, v_t = (jnp.transpose(a[0, :, 0, :]) for a in (q_saved, k_saved, v_saved))
        w_qkv_t = jnp.transpose(w_qkv[:, :, 0, :], (0, 2, 1)).reshape(3 * dim, -1)
        dw1, dw2, db1, dwo, dx, dw_t, db, vecs = layer_stage(
            n, d_out[0], x_mid[0], z_saved[0], w_fc1, w_fc2, q_t, k_t, v_t, w_proj[0], x_in[0], w_qkv_t,
            row(ln2_gain), row(ln2_bias), row(ln1_gain), row(ln1_bias))
        dw1, dw2, dwo, dw_t, dx, db1, db, vecs = deliver((dw1, dw2, dwo, dw_t, dx, db1, db, vecs))
        grad_wqkv = jnp.transpose(dw_t.reshape(3, dim, -1), (0, 2, 1))[:, :, None, :]
        return dx[None], grad_wqkv, db, dwo[None], dw1, db1[0], dw2, vecs

    tok_spec = P('dp', 'tp', None)
    head_spec = P('dp', None, 'tp', None)
    in_specs = (tok_spec, tok_spec, tok_spec, head_spec, head_spec, head_spec, P('dp', None, 'tp'),
                P(None), P(None), P(None), P(None),
                P(None, None, 'tp', None), P('tp', None, None), P(None, 'tp'), P('tp', None))
    out_specs = (tok_spec, P('dp', None, 'tp', None), P('dp', 'tp', None), P(('dp', 'tp'), None, None),
                 P('dp', 'tp'), P(('dp', 'tp')), P(('dp', 'tp'), None), P('dp', None))
    return jax.shard_map(local_backward, mesh=mesh, in_specs=in_specs, out_specs=out_specs, check_vma=False)
```
